32 devices in a mesh: dp: 1 (over z), ctx: 32 (over y, x, core).
Axes of the slice: x: 4, y: 4, z: 1, core: 2. Of those that a mesh axis runs over, the one named last changes fastest.
The devices are a block of a 4x4x8 slice.
Arguments:
- q_seq: bfloat16 [1, 8192, 16, 128], P('dp', 'ctx')
- k_seq: bfloat16 [1, 8192, 4, 128], P('dp', 'ctx')
- v_seq: bfloat16 [1, 8192, 4, 128], P('dp', 'ctx')
- do_seq: bfloat16 [1, 8192, 16, 128], P('dp', 'ctx')
Outputs:
- output 1: bfloat16 [1, 8192, 16, 128], P('dp', 'ctx')
- output 2: bfloat16 [1, 8192, 16, 128], P('dp', 'ctx')
- output 3: bfloat16 [1, 8192, 4, 128], P('dp', 'ctx')
- output 4: bfloat16 [1, 8192, 4, 128], P('dp', 'ctx')
All inputs are finite; a program needn't handle non-finite values.
Results may differ from the reference program's by a relative error of at most 0.00873153.
Values are sent between devices in bfloat16 or wider.
A program may use at most 768 MiB of HBM per device.

```python
import math
import jax
import jax.numpy as jnp
from jax import lax

BATCH = 1
CTX = 32
CHUNK = 256
Q_HEADS = 16
KV_LOCAL = 4
HEAD = 128
WINDOW = 4096

SEQ = CTX * CHUNK
GROUP = Q_HEADS // KV_LOCAL
QBLK = min(CHUNK, 128)
NEG_BIG = -1e30


def setup_inputs(seed: int = 0, part: int = 0) -> dict:
    base_key = jax.random.fold_in(jax.random.key(seed), part)
    key_q, key_k, key_v, key_do = jax.random.split(base_key, 4)
    input_std = (0.5 * math.log(WINDOW)) ** 0.25
    q_shape = (BATCH, SEQ, Q_HEADS, HEAD)
    kv_shape = (BATCH, SEQ, KV_LOCAL, HEAD)
    q_seq = input_std * jax.random.normal(key_q, q_shape, jnp.float32)
    k_seq = input_std * jax.random.normal(key_k, kv_shape, jnp.float32)
    v_seq = jax.random.normal(key_v, kv_shape, jnp.float32)
    do_seq = jax.random.normal(key_do, q_shape, jnp.float32)
    return {'q_seq': q_seq.astype(jnp.bfloat16), 'k_seq': k_seq.astype(jnp.bfloat16), 'v_seq': v_seq.astype(jnp.bfloat16), 'do_seq': do_seq.astype(jnp.bfloat16)}


def attend_all(q_full, k_full, v_full):
    n_blk = SEQ // QBLK
    q_blocks = jnp.moveaxis(q_full.reshape(BATCH, n_blk, QBLK, KV_LOCAL, GROUP, HEAD), 1, 0)
    pad_width = ((0, 0), (WINDOW, 0), (0, 0), (0, 0))
    k_pad = jnp.pad(k_full, pad_width)
    v_pad = jnp.pad(v_full, pad_width)
    span_len = WINDOW + QBLK
    dist = jnp.arange(QBLK)[:, None] + WINDOW - jnp.arange(span_len)[None, :]
    pair_ok = (dist >= 0) & (dist < WINDOW)
    sm_scale = HEAD ** -0.5

    def one_block(blk_args):
        blk_id, q_blk = blk_args
        start = blk_id * QBLK
        k_win = lax.dynamic_slice_in_dim(k_pad, start, span_len, axis=1)
        v_win = lax.dynamic_slice_in_dim(v_pad, start, span_len, axis=1)
        keep_mask = pair_ok & (jnp.arange(span_len)[None, :] + start >= WINDOW)
        scores = jnp.einsum('bqhgd,bkhd->bhgqk', q_blk, k_win) * sm_scale
        scores = jnp.where(keep_mask, scores, NEG_BIG)
        weights = jax.nn.softmax(scores, axis=-1)
        return jnp.einsum('bhgqk,bkhd->bqhgd', weights, v_win)

    o_blocks = lax.map(jax.checkpoint(one_block), (jnp.arange(n_blk), q_blocks))
    return jnp.moveaxis(o_blocks, 0, 1).reshape(BATCH, SEQ, Q_HEADS, HEAD)


def reference(q_seq, k_seq, v_seq, do_seq):
    o_full, pull_back = jax.vjp(attend_all, q_seq.astype(jnp.float32), k_seq.astype(jnp.float32), v_seq.astype(jnp.float32))
    dq_full, dk_full, dv_full = pull_back(do_seq.astype(jnp.float32))
    return (o_full.astype(jnp.bfloat16), dq_full.astype(jnp.bfloat16), dk_full.astype(jnp.bfloat16), dv_full.astype(jnp.bfloat16))
```

```python
import functools

import jax
import jax.numpy as jnp
from jax import lax
from jax.experimental import pallas as pl
from jax.experimental.pallas import tpu as pltpu
from jax.sharding import PartitionSpec as P

WINDOW = 4096
NEG = -1e30
LOG2E = 1.4426950408889634
F32 = jnp.float32
BF16 = jnp.bfloat16


def dot(a, b):
    return jnp.dot(a, b, preferred_element_type=F32)


def fold8(x, op):
    n = x.shape[0] // 8
    acc = x[0:8]
    for t in range(1, n):
        acc = op(acc, x[8 * t:8 * t + 8])
    return acc


def attn_kernel(inner, n_win, sm_scale, q_ref, do_ref, k_ref, v_ref, o_ref, dq_ref, dk_ref, dv_ref,
                kt, vt, qt, dot_t, s_scr, acc_t, m_scr, l_scr, lse_scr, d_scr):
    n_q, group, chunk, dim = q_ref.shape
    n_kv = k_ref.shape[0]
    row_pos = lax.rem(lax.axis_index('ctx'), inner)
    c_exp = sm_scale * LOG2E

    def prep(j, _):
        kt[j] = k_ref[j].T
        vt[j] = v_ref[j].T
        dk_ref[j] = jnp.zeros((chunk, dim), F32)
        dv_ref[j] = jnp.zeros((chunk, dim), F32)
        return 0

    lax.fori_loop(0, n_kv, prep, 0)
    rows = lax.broadcasted_iota(jnp.int32, (chunk, chunk), 0)
    cols = lax.broadcasted_iota(jnp.int32, (chunk, chunk), 1)

    def cs(h):
        return slice(h * chunk, (h + 1) * chunk)

    def one_chunk(i, _):
        g = i * inner + row_pos
        lo = jnp.maximum(g - n_win, 0)
        n = g - lo + 1
        for h in range(group):
            qt[:, cs(h)] = q_ref[i, h].T
            dot_t[:, cs(h)] = do_ref[i, h].T
        m_scr[...] = jnp.full(m_scr.shape, NEG, F32)
        l_scr[...] = jnp.zeros(l_scr.shape, F32)

        def score(jj, keep):
            kb = k_ref[lo + jj]
            for h in range(group):
                s = dot(kb, qt[:, cs(h)])
                if keep is not None:
                    s = jnp.where(keep, s, NEG)
                s_scr[jj, :, cs(h)] = s
                m_scr[:, cs(h)] = jnp.maximum(m_scr[:, cs(h)], fold8(s, jnp.maximum))

        old_edge = g >= n_win
        first = jnp.where(old_edge, 1, 0)

        @pl.when(old_edge)
        def _():
            score(0, rows > cols)

        def score_body(jj, _):
            score(jj, None)
            return 0

        lax.fori_loop(first, n - 1, score_body, 0)
        score(n - 1, rows <= cols)
        m_row = jnp.max(m_scr[...], axis=0, keepdims=True) * c_exp
        m_scr[...] = jnp.broadcast_to(m_row, m_scr.shape)
        acc_t[...] = jnp.zeros(acc_t.shape, F32)

        def pv_body(jj, _):
            vb = vt[lo + jj]
            for h in range(group):
                p = jnp.exp2(s_scr[jj, :, cs(h)] * c_exp - m_scr[0:1, cs(h)])
                l_scr[:, cs(h)] += fold8(p, jnp.add)
                acc_t[:, cs(h)] += dot(vb, p.astype(BF16))
            return 0

        lax.fori_loop(0, n, pv_body, 0)
        l_row = jnp.sum(l_scr[...], axis=0, keepdims=True)
        lse_scr[...] = jnp.broadcast_to(m_scr[0:1] + jnp.log2(l_row), lse_scr.shape)
        for h in range(group):
            o_t = (acc_t[:, cs(h)] / l_row[:, cs(h)]).astype(BF16)
            d = jnp.sum(o_t.astype(F32) * dot_t[:, cs(h)].astype(F32), axis=0, keepdims=True)
            d_scr[:, cs(h)] = jnp.broadcast_to(d, (8, chunk))
            o_ref[i, h] = o_t.T
        acc_t[...] = jnp.zeros(acc_t.shape, F32)

        def bwd_body(jj, _):
            j = lo + jj
            vb = v_ref[j]
            kb = kt[j]
            dv = dv_ref[j]
            dk = dk_ref[j]
            for h in range(group):
                p = jnp.exp2(s_scr[jj, :, cs(h)] * c_exp - lse_scr[0:1, cs(h)])
                dp = dot(vb, dot_t[:, cs(h)])
                ds = (p * (dp - d_scr[0:1, cs(h)])).astype(BF16)
                dv = dv + dot(p.astype(BF16), do_ref[i, h])
                dk = dk + dot(ds, q_ref[i, h])
                acc_t[:, cs(h)] += dot(kb, ds)
            dv_ref[j] = dv
            dk_ref[j] = dk
            return 0

        lax.fori_loop(0, n, bwd_body, 0)
        for h in range(group):
            dq_ref[i, h] = (acc_t[:, cs(h)] * sm_scale).astype(BF16).T
        return 0

    lax.fori_loop(0, n_q, one_chunk, 0)


def solution(mesh):
    n_ctx = mesh.shape['ctx']
    seq_spec = P('dp', 'ctx', None, None)

    def local_attn(q_loc, k_loc, v_loc, do_loc):
        n_batch, chunk, q_heads, dim = q_loc.shape
        kv_heads = k_loc.shape[2]
        group = q_heads // kv_heads
        inner = n_ctx // kv_heads
        n_win = WINDOW // chunk
        n_q = kv_heads
        cols = [[y * inner + r for y in range(kv_heads)] for r in range(inner)]
        rows = [[y * inner + r for r in range(inner)] for y in range(kv_heads)]

        def split(x, per):
            x = jnp.transpose(x[0], (1, 0, 2)).reshape(kv_heads, per, chunk, dim)
            return lax.all_to_all(x, 'ctx', 0, 0, axis_index_groups=cols)

        def merge(x, per):
            x = lax.all_to_all(x, 'ctx', 0, 0, axis_index_groups=cols)
            return jnp.transpose(x.reshape(kv_heads * per, chunk, dim), (1, 0, 2))[None]

        q4, do4 = split(q_loc, group), split(do_loc, group)
        k4, v4 = split(k_loc, 1), split(v_loc, 1)
        k_all = lax.all_gather(k4[:, 0], 'ctx', axis_index_groups=rows, axis=1).reshape(n_ctx, chunk, dim)
        v_all = lax.all_gather(v4[:, 0], 'ctx', axis_index_groups=rows, axis=1).reshape(n_ctx, chunk, dim)
        wide = group * chunk
        vm = pl.BlockSpec(memory_space=pltpu.VMEM)
        o4, dq4, dk, dv = pl.pallas_call(
            functools.partial(attn_kernel, inner, n_win, dim ** -0.5),
            out_shape=(jax.ShapeDtypeStruct(q4.shape, BF16), jax.ShapeDtypeStruct(q4.shape, BF16),
                       jax.ShapeDtypeStruct(k_all.shape, F32), jax.ShapeDtypeStruct(k_all.shape, F32)),
            in_specs=[vm] * 4,
            out_specs=(vm,) * 4,
            scratch_shapes=[
                pltpu.VMEM((n_ctx, dim, chunk), BF16), pltpu.VMEM((n_ctx, dim, chunk), BF16),
                pltpu.VMEM((dim, wide), BF16), pltpu.VMEM((dim, wide), BF16),
                pltpu.VMEM((n_win + 1, chunk, wide), F32), pltpu.VMEM((dim, wide), F32),
                pltpu.VMEM((8, wide), F32), pltpu.VMEM((8, wide), F32),
                pltpu.VMEM((8, wide), F32), pltpu.VMEM((8, wide), F32),
            ],
            compiler_params=pltpu.CompilerParams(vmem_limit_bytes=60 * 1024 * 1024),
            name='attn_core',
        )(q4, do4, k_all, v_all)
        sm_scale = dim ** -0.5

        def reduce(x):
            x = lax.psum_scatter(x.reshape(n_q, inner, chunk, dim), 'ctx', scatter_dimension=1, axis_index_groups=rows)
            return x[:, None]

        dk4 = (reduce(dk) * sm_scale).astype(BF16)
        dv4 = reduce(dv).astype(BF16)
        return merge(o4, group), merge(dq4, group), merge(dk4, 1), merge(dv4, 1)

    return jax.shard_map(local_attn, mesh=mesh, in_specs=(seq_spec,) * 4, out_specs=(seq_spec,) * 4, check_vma=False)
```

```python
import functools

import jax
import jax.numpy as jnp
from jax import lax
from jax.experimental import pallas as pl
from jax.experimental.pallas import tpu as pltpu
from jax.sharding import PartitionSpec as P

WINDOW = 4096
NEG = -1e30
LOG2E = 1.4426950408889634
F32 = jnp.float32
BF16 = jnp.bfloat16


def dot(a, b):
    return jnp.dot(a, b, preferred_element_type=F32)


def fold8(x, op):
    n = x.shape[0] // 8
    acc = x[0:8]
    for t in range(1, n):
        acc = op(acc, x[8 * t:8 * t + 8])
    return acc


MESH = pl.DeviceIdType.MESH


def attn_kernel(inner, n_win, sm_scale, q_loc, do_loc, kv_loc, o_out, dq_out, dkv_out,
                q_all, do_all, kv_all, kt, vt, qt, dot_t, s_scr, acc_t, m_scr, l_scr, lse_scr, d_scr,
                dkv, o_st, dq_st, sib_in, x_in, dkv_st,
                loc_sem, in_s, in_r, ag_s, ag_r, sb_s, sb_r, od_s, od_r, ds_s, ds_r, xs_s, xs_r, fy_s, fy_r):
    n_y, group, chunk, dim = q_loc.shape
    n_kv = kv_all.shape[0]
    n_x = inner // 2
    half = n_kv // 2
    dp = lax.axis_index('dp')
    me = lax.axis_index('ctx')
    y, r = me // inner, lax.rem(me, inner)
    x, c = r // 2, lax.rem(r, 2)
    c_exp = sm_scale * LOG2E

    def dev(yy, xx, cc):
        return (dp, yy * inner + xx * 2 + cc)

    def y_at(dy):
        return lax.rem(y + dy + n_y, n_y)

    def x_at(dx):
        return lax.rem(x + dx + n_x, n_x)

    def rcopy(src, dst, s, rr, to):
        return pltpu.make_async_remote_copy(src_ref=src, dst_ref=dst, send_sem=s, recv_sem=rr, device_id=to, device_id_type=MESH)

    sib = dev(y, x, 1 - c)
    peers = [dev(y_at(d), x, c) for d in range(1, n_y)] + [dev(y, x_at(d), c) for d in range(1, n_x)] + [sib]
    barrier = pltpu.get_barrier_semaphore()
    for p in peers:
        pl.semaphore_signal(barrier, inc=1, device_id=p, device_id_type=MESH)
    pl.semaphore_wait(barrier, len(peers))

    mine = y * inner + r
    locs = [pltpu.make_async_copy(kv_loc.at[y], kv_all.at[mine], loc_sem.at[0]),
            pltpu.make_async_copy(q_loc.at[y], q_all.at[y], loc_sem.at[1]),
            pltpu.make_async_copy(do_loc.at[y], do_all.at[y], loc_sem.at[2])]
    for cp in locs:
        cp.start()
    order = [1, n_y - 1] + list(range(2, n_y - 1))
    ins = []
    for k, (src, dst, at) in enumerate(((kv_loc, kv_all, mine), (q_loc, q_all, y), (do_loc, do_all, y))):
        for d in order:
            cp = rcopy(src.at[y_at(d)], dst.at[at], in_s.at[k, d], in_r.at[k, d], dev(y_at(d), x, c))
            cp.start()
            ins.append(cp)

    def fwd_sib(slot, dx, idx):
        cp = rcopy(kv_all.at[idx], kv_all.at[idx], sb_s.at[slot, dx], sb_r.at[slot, dx], sib)
        cp.start()
        return cp

    xorder = [1, n_x - 1] + list(range(2, n_x - 1))
    ags, sbs = [], []
    for d in [0] + order:
        own = y_at(-d) * inner + r
        if d == 0:
            locs[0].wait()
        else:
            rcopy(kv_loc.at[y], kv_all.at[own], in_s.at[0, d], in_r.at[0, d], sib).wait_recv()
        for dx in xorder:
            cp = rcopy(kv_all.at[own], kv_all.at[own], ag_s.at[d, dx], ag_r.at[d, dx], dev(y, x_at(dx), c))
            cp.start()
            ags.append(cp)
        sbs.append(fwd_sib(d, 0, own))
    for d in [0] + order:
        for dx in xorder:
            idx = y_at(-d) * inner + x_at(-dx) * 2 + c
            rcopy(kv_all.at[idx], kv_all.at[idx], ag_s.at[d, dx], ag_r.at[d, dx], sib).wait_recv()
            sbs.append(fwd_sib(d, dx, idx))
    for d in [0] + order:
        for dx in [0] + xorder:
            idx = y_at(-d) * inner + x_at(-dx) * 2 + 1 - c
            rcopy(kv_all.at[idx], kv_all.at[idx], sb_s.at[d, dx], sb_r.at[d, dx], sib).wait_recv()
    for k, dst, loc in ((1, q_all, locs[1]), (2, do_all, locs[2])):
        loc.wait()
        for d in order:
            at = y_at(-d)
            rcopy(dst.at[at], dst.at[at], in_s.at[k, d], in_r.at[k, d], sib).wait_recv()
    for cp in ins + ags + sbs:
        cp.wait_send()

    def prep(j, _):
        kt[j] = kv_all[j, 0].T
        vt[j] = kv_all[j, 1].T
        dkv[j] = jnp.zeros((2, chunk, dim), F32)
        return 0

    lax.fori_loop(0, n_kv, prep, 0)
    rows = lax.broadcasted_iota(jnp.int32, (chunk, chunk), 0)
    cols = lax.broadcasted_iota(jnp.int32, (chunk, chunk), 1)

    def cs(h):
        return slice(h * chunk, (h + 1) * chunk)

    def out_copies(i):
        return [rcopy(st.at[i], out.at[y], od_s.at[k, i], od_r.at[k, y], dev(i, x, c))
                for k, (st, out) in enumerate(((o_st, o_out), (dq_st, dq_out)))]

    def one_chunk(step, _):
        i = n_y - 1 - step
        g = i * inner + r
        lo = jnp.maximum(g - n_win, 0)
        n = g - lo + 1
        for h in range(group):
            qt[:, cs(h)] = q_all[i, h].T
            dot_t[:, cs(h)] = do_all[i, h].T
        m_scr[...] = jnp.full(m_scr.shape, NEG, F32)
        l_scr[...] = jnp.zeros(l_scr.shape, F32)

        def score(jj, keep):
            kb = kv_all[lo + jj, 0]
            for h in range(group):
                s = dot(kb, qt[:, cs(h)])
                if keep is not None:
                    s = jnp.where(keep, s, NEG)
                s_scr[jj, :, cs(h)] = s
                m_scr[:, cs(h)] = jnp.maximum(m_scr[:, cs(h)], fold8(s, jnp.maximum))

        old_edge = g >= n_win
        first = jnp.where(old_edge, 1, 0)

        @pl.when(old_edge)
        def _():
            score(0, rows > cols)

        def score_body(jj, _):
            score(jj, None)
            return 0

        lax.fori_loop(first, n - 1, score_body, 0)
        score(n - 1, rows <= cols)
        m_row = jnp.max(m_scr[...], axis=0, keepdims=True) * c_exp
        m_scr[...] = jnp.broadcast_to(m_row, m_scr.shape)
        acc_t[...] = jnp.zeros(acc_t.shape, F32)

        def pv_body(jj, _):
            vb = vt[lo + jj]
            for h in range(group):
                p = jnp.exp2(s_scr[jj, :, cs(h)] * c_exp - m_scr[0:1, cs(h)])
                l_scr[:, cs(h)] += fold8(p, jnp.add)
                acc_t[:, cs(h)] += dot(vb, p.astype(BF16))
            return 0

        lax.fori_loop(0, n, pv_body, 0)
        l_row = jnp.sum(l_scr[...], axis=0, keepdims=True)
        lse_scr[...] = jnp.broadcast_to(m_scr[0:1] + jnp.log2(l_row), lse_scr.shape)
        for h in range(group):
            o_t = (acc_t[:, cs(h)] / l_row[:, cs(h)]).astype(BF16)
            d = jnp.sum(o_t.astype(F32) * dot_t[:, cs(h)].astype(F32), axis=0, keepdims=True)
            d_scr[:, cs(h)] = jnp.broadcast_to(d, (8, chunk))
            o_st[i, h] = o_t.T
        acc_t[...] = jnp.zeros(acc_t.shape, F32)

        @pl.when(i != y)
        def _():
            out_copies(i)[0].start()

        def bwd_body(jj, _):
            j = lo + jj
            at = lax.rem(j, 2) * half + j // 2
            vb = kv_all[j, 1]
            kb = kt[j]
            dk = dkv[at, 0]
            dv = dkv[at, 1]
            for h in range(group):
                p = jnp.exp2(s_scr[jj, :, cs(h)] * c_exp - lse_scr[0:1, cs(h)])
                dp_t = dot(vb, dot_t[:, cs(h)])
                ds = (p * (dp_t - d_scr[0:1, cs(h)])).astype(BF16)
                dv = dv + dot(p.astype(BF16), do_all[i, h])
                dk = dk + dot(ds, q_all[i, h])
                acc_t[:, cs(h)] += dot(kb, ds)
            dkv[at, 0] = dk
            dkv[at, 1] = dv
            return 0

        lax.fori_loop(0, n, bwd_body, 0)
        for h in range(group):
            dq_st[i, h] = (acc_t[:, cs(h)] * sm_scale).astype(BF16).T

        @pl.when(i != y)
        def _():
            out_copies(i)[1].start()

        return 0

    lax.fori_loop(0, n_y, one_chunk, 0)
    o_out[y] = o_st[y]
    dq_out[y] = dq_st[y]

    def sib_copy(i):
        return rcopy(dkv.at[pl.ds((1 - c) * half + n_x * i, n_x)], sib_in.at[pl.ds(n_x * i, n_x)], ds_s.at[i], ds_r.at[i], sib)

    def x_copy(i, dx):
        return rcopy(dkv.at[c * half + n_x * i + x_at(dx)], x_in.at[dx, i], xs_s.at[i, dx], xs_r.at[i, dx], dev(y, x_at(dx), c))

    def y_copy(i):
        return rcopy(dkv_st.at[i], dkv_out.at[y], fy_s.at[i], fy_r.at[y], dev(i, x, c))

    slots = list(range(n_y - 1, -1, -1))
    for i in slots:
        sib_copy(i).start()
    for i in slots:
        sib_copy(i).wait_recv()

        def add(t, _):
            at = c * half + n_x * i + t
            dkv[at] = dkv[at] + sib_in[n_x * i + t]
            return 0

        lax.fori_loop(0, n_x, add, 0)
        for dx in xorder:
            x_copy(i, dx).start()
    for i in slots:
        for dx in xorder:
            x_copy(i, dx).wait_recv()
        tot = dkv[c * half + n_x * i + x]
        for dx in xorder:
            tot = tot + x_in[dx, i]
        dkv_st[i, 0] = (tot[0] * sm_scale).astype(BF16)
        dkv_st[i, 1] = tot[1].astype(BF16)

        @pl.when(i != y)
        def _():
            y_copy(i).start()

    dkv_out[y] = dkv_st[y]
    for yy in range(n_y):
        @pl.when(yy != y)
        def _():
            for k, out in enumerate((o_out, dq_out)):
                rcopy(o_st.at[yy], out.at[yy], od_s.at[k, yy], od_r.at[k, yy], sib).wait_recv()
            rcopy(dkv_st.at[yy], dkv_out.at[yy], fy_s.at[yy], fy_r.at[yy], sib).wait_recv()
            for cp in out_copies(yy):
                cp.wait_send()
            y_copy(yy).wait_send()

        sib_copy(yy).wait_send()
        for dx in xorder:
            x_copy(yy, dx).wait_send()


def solution(mesh):
    n_ctx = mesh.shape['ctx']
    seq_spec = P('dp', 'ctx', None, None)

    def local_attn(q_loc, k_loc, v_loc, do_loc):
        n_batch, chunk, q_heads, dim = q_loc.shape
        kv_heads = k_loc.shape[2]
        group = q_heads // kv_heads
        inner = n_ctx // kv_heads
        n_x = inner // 2
        n_win = WINDOW // chunk
        n_y = kv_heads
        wide = group * chunk

        def heads(x, per):
            return jnp.transpose(x[0], (1, 0, 2)).reshape(kv_heads, per, chunk, dim)

        def tokens(x):
            return jnp.transpose(x.reshape(-1, chunk, dim), (1, 0, 2))[None]

        q4, do4 = heads(q_loc, group), heads(do_loc, group)
        kv4 = jnp.concatenate([heads(k_loc, 1), heads(v_loc, 1)], axis=1)
        vm = pl.BlockSpec(memory_space=pltpu.VMEM)
        dma = pltpu.SemaphoreType.DMA
        o4, dq4, dkv4 = pl.pallas_call(
            functools.partial(attn_kernel, inner, n_win, dim ** -0.5),
            out_shape=(jax.ShapeDtypeStruct(q4.shape, BF16), jax.ShapeDtypeStruct(q4.shape, BF16),
                       jax.ShapeDtypeStruct(kv4.shape, BF16)),
            in_specs=[vm] * 3,
            out_specs=(vm,) * 3,
            scratch_shapes=[
                pltpu.VMEM(q4.shape, BF16), pltpu.VMEM(q4.shape, BF16), pltpu.VMEM((n_ctx, 2, chunk, dim), BF16),
                pltpu.VMEM((n_ctx, dim, chunk), BF16), pltpu.VMEM((n_ctx, dim, chunk), BF16),
                pltpu.VMEM((dim, wide), BF16), pltpu.VMEM((dim, wide), BF16),
                pltpu.VMEM((n_win + 1, chunk, wide), F32), pltpu.VMEM((dim, wide), F32),
                pltpu.VMEM((8, wide), F32), pltpu.VMEM((8, wide), F32),
                pltpu.VMEM((8, wide), F32), pltpu.VMEM((8, wide), F32),
                pltpu.VMEM((n_ctx, 2, chunk, dim), F32), pltpu.VMEM(q4.shape, BF16), pltpu.VMEM(q4.shape, BF16),
                pltpu.VMEM((n_ctx // 2, 2, chunk, dim), F32), pltpu.VMEM((n_x, n_y, 2, chunk, dim), F32),
                pltpu.VMEM(kv4.shape, BF16),
                dma((3,)), dma((3, n_y)), dma((3, n_y)), dma((n_y, n_x)), dma((n_y, n_x)), dma((n_y, n_x)), dma((n_y, n_x)),
                dma((2, n_y)), dma((2, n_y)), dma((n_y,)), dma((n_y,)), dma((n_y, n_x)), dma((n_y, n_x)),
                dma((n_y,)), dma((n_y,)),
            ],
            compiler_params=pltpu.CompilerParams(vmem_limit_bytes=63 * 1024 * 1024, collective_id=0, has_side_effects=True),
            name='attn_core',
        )(q4, do4, kv4)
        return tokens(o4), tokens(dq4), tokens(dkv4[:, 0]), tokens(dkv4[:, 1])

    return jax.shard_map(local_attn, mesh=mesh, in_specs=(seq_spec,) * 4, out_specs=(seq_spec,) * 4, check_vma=False)
```

```python
import functools

import jax
import jax.numpy as jnp
from jax import lax
from jax.experimental import pallas as pl
from jax.experimental.pallas import tpu as pltpu
from jax.sharding import PartitionSpec as P

WINDOW = 4096
NEG = -1e30
LOG2E = 1.4426950408889634
F32 = jnp.float32
BF16 = jnp.bfloat16


def dot(a, b):
    return jnp.dot(a, b, preferred_element_type=F32)


def fold8(x, op):
    n = x.shape[0] // 8
    acc = x[0:8]
    for t in range(1, n):
        acc = op(acc, x[8 * t:8 * t + 8])
    return acc


MESH = pl.DeviceIdType.MESH


def attn_kernel(inner, n_win, sm_scale, q_loc, do_loc, kv_loc, o_out, dq_out, dkv_out,
                q_all, do_all, kv_all, kt, vt, qt, dot_t, s_scr, acc_t, m_scr, l_scr, lse_scr, d_scr,
                dkv, o_st, dq_st, sib_in, x_in, dkv_st,
                loc_sem, in_s, in_r, ag_s, ag_r, sb_s, sb_r, od_s, od_r, ds_s, ds_r, xs_s, xs_r, fy_s, fy_r):
    n_y, group, chunk, dim = q_loc.shape
    n_kv = kv_all.shape[0]
    n_x = inner // 2
    half = n_kv // 2
    dp = lax.axis_index('dp')
    me = lax.axis_index('ctx')
    y, r = me // inner, lax.rem(me, inner)
    x, c = r // 2, lax.rem(r, 2)
    c_exp = sm_scale * LOG2E

    def dev(yy, xx, cc):
        return (dp, yy * inner + xx * 2 + cc)

    def y_at(dy):
        return lax.rem(y + dy + n_y, n_y)

    def x_at(dx):
        return lax.rem(x + dx + n_x, n_x)

    def rcopy(src, dst, s, rr, to):
        return pltpu.make_async_remote_copy(src_ref=src, dst_ref=dst, send_sem=s, recv_sem=rr, device_id=to, device_id_type=MESH)

    sib = dev(y, x, 1 - c)
    peers = [dev(y_at(d), x, c) for d in range(1, n_y)] + [dev(y, x_at(d), c) for d in range(1, n_x)] + [sib]
    barrier = pltpu.get_barrier_semaphore()
    for p in peers:
        pl.semaphore_signal(barrier, inc=1, device_id=p, device_id_type=MESH)
    pl.semaphore_wait(barrier, len(peers))

    mine = y * inner + r
    locs = [pltpu.make_async_copy(kv_loc.at[y], kv_all.at[mine], loc_sem.at[0]),
            pltpu.make_async_copy(q_loc.at[y], q_all.at[y], loc_sem.at[1]),
            pltpu.make_async_copy(do_loc.at[y], do_all.at[y], loc_sem.at[2])]
    for cp in locs:
        cp.start()
    order = [1, n_y - 1] + list(range(2, n_y - 1))
    ins = []
    for k, (src, dst, at) in enumerate(((kv_loc, kv_all, mine), (q_loc, q_all, y), (do_loc, do_all, y))):
        for d in order:
            cp = rcopy(src.at[y_at(d)], dst.at[at], in_s.at[k, d], in_r.at[k, d], dev(y_at(d), x, c))
            cp.start()
            ins.append(cp)

    def fwd_sib(slot, dx, idx):
        cp = rcopy(kv_all.at[idx], kv_all.at[idx], sb_s.at[slot, dx], sb_r.at[slot, dx], sib)
        cp.start()
        return cp

    xorder = [1, n_x - 1] + list(range(2, n_x - 1))
    ags, sbs = [], []
    for d in [0] + order:
        own = y_at(-d) * inner + r
        if d == 0:
            locs[0].wait()
        else:
            rcopy(kv_loc.at[y], kv_all.at[own], in_s.at[0, d], in_r.at[0, d], sib).wait_recv()
        for dx in xorder:
            cp = rcopy(kv_all.at[own], kv_all.at[own], ag_s.at[d, dx], ag_r.at[d, dx], dev(y, x_at(dx), c))
            cp.start()
            ags.append(cp)
        sbs.append(fwd_sib(d, 0, own))
    for d in [0] + order:
        for dx in xorder:
            idx = y_at(-d) * inner + x_at(-dx) * 2 + c
            rcopy(kv_all.at[idx], kv_all.at[idx], ag_s.at[d, dx], ag_r.at[d, dx], sib).wait_recv()
            sbs.append(fwd_sib(d, dx, idx))
    for d in [0] + order:
        for dx in [0] + xorder:
            idx = y_at(-d) * inner + x_at(-dx) * 2 + 1 - c
            rcopy(kv_all.at[idx], kv_all.at[idx], sb_s.at[d, dx], sb_r.at[d, dx], sib).wait_recv()
    for k, dst, loc in ((1, q_all, locs[1]), (2, do_all, locs[2])):
        loc.wait()
        for d in order:
            at = y_at(-d)
            rcopy(dst.at[at], dst.at[at], in_s.at[k, d], in_r.at[k, d], sib).wait_recv()
    for cp in ins + ags + sbs:
        cp.wait_send()

    def prep(j, _):
        kt[j] = kv_all[j, 0].T
        vt[j] = kv_all[j, 1].T
        dkv[j] = jnp.zeros((2, chunk, dim), F32)
        return 0

    lax.fori_loop(0, n_kv, prep, 0)
    rows = lax.broadcasted_iota(jnp.int32, (chunk, chunk), 0)
    cols = lax.broadcasted_iota(jnp.int32, (chunk, chunk), 1)

    def cs(h):
        return slice(h * chunk, (h + 1) * chunk)

    def out_copies(i):
        return [rcopy(st.at[i], out.at[y], od_s.at[k, i], od_r.at[k, y], dev(i, x, c))
                for k, (st, out) in enumerate(((o_st, o_out), (dq_st, dq_out)))]

    def one_chunk(step, _):
        i = n_y - 1 - step
        g = i * inner + r
        lo = jnp.maximum(g - n_win, 0)
        n = g - lo + 1
        for h in range(group):
            qt[:, cs(h)] = q_all[i, h].T
            dot_t[:, cs(h)] = do_all[i, h].T
        m_scr[...] = jnp.full(m_scr.shape, NEG, F32)
        l_scr[...] = jnp.zeros(l_scr.shape, F32)
        acc_t[...] = jnp.zeros(acc_t.shape, F32)

        def fwd(blocks):
            def score(h):
                return [dot(kv_all[lo + jj, 0], qt[:, cs(h)]) for jj, _ in blocks]

            nxt = score(0)
            for h in range(group):
                cur = nxt
                if h + 1 < group:
                    nxt = score(h + 1)
                m_old = m_scr[:, cs(h)]
                mx = m_old
                for (jj, keep), s in zip(blocks, cur):
                    s = s * c_exp
                    if keep is not None:
                        s = jnp.where(keep, s, NEG)
                    s_scr[jj, :, cs(h)] = s
                    mx = jnp.maximum(mx, fold8(s, jnp.maximum))
                m_new = jnp.broadcast_to(jnp.max(mx, axis=0, keepdims=True), m_old.shape)
                alpha = jnp.exp2(m_old - m_new)
                m_scr[:, cs(h)] = m_new
                l_new = l_scr[:, cs(h)] * alpha
                pv = None
                for jj, _ in blocks:
                    p = jnp.exp2(s_scr[jj, :, cs(h)] - m_new[0:1])
                    l_new = l_new + fold8(p, jnp.add)
                    part = dot(vt[lo + jj], p.astype(BF16))
                    pv = part if pv is None else pv + part
                l_scr[:, cs(h)] = l_new
                acc_t[:, cs(h)] = acc_t[:, cs(h)] * alpha[0:1] + pv

        old_edge = g >= n_win
        first = jnp.where(old_edge, 1, 0)
        n_mid = n - 1 - first

        @pl.when(old_edge)
        def _():
            fwd([(0, rows > cols), (n - 1, rows <= cols)])

        @pl.when(jnp.logical_not(old_edge))
        def _():
            fwd([(n - 1, rows <= cols)])

        def fwd_body(t, _):
            fwd([(first + 2 * t, None), (first + 2 * t + 1, None)])
            return 0

        lax.fori_loop(0, n_mid // 2, fwd_body, 0)

        @pl.when(lax.rem(n_mid, 2) == 1)
        def _():
            fwd([(first + n_mid - 1, None)])

        l_row = jnp.sum(l_scr[...], axis=0, keepdims=True)
        lse_scr[...] = jnp.broadcast_to(m_scr[0:1] + jnp.log2(l_row), lse_scr.shape)
        for h in range(group):
            o_t = (acc_t[:, cs(h)] / l_row[:, cs(h)]).astype(BF16)
            d = jnp.sum(o_t.astype(F32) * dot_t[:, cs(h)].astype(F32), axis=0, keepdims=True)
            d_scr[:, cs(h)] = jnp.broadcast_to(d, (8, chunk))
            o_st[i, h] = o_t.T
        acc_t[...] = jnp.zeros(acc_t.shape, F32)

        @pl.when(i != y)
        def _():
            out_copies(i)[0].start()

        def bwd(jjs):
            units = [(b, h) for b in range(len(jjs)) for h in range(group)]
            at_j = [lo + jj for jj in jjs]
            at = [lax.rem(j, 2) * half + j // 2 for j in at_j]

            def grad_p(b, h):
                return dot(kv_all[at_j[b], 1], dot_t[:, cs(h)])

            nxt = grad_p(*units[0])
            dk = dv = None
            for k, (b, h) in enumerate(units):
                cur = nxt
                if k + 1 < len(units):
                    nxt = grad_p(*units[k + 1])
                p = jnp.exp2(s_scr[jjs[b], :, cs(h)] - lse_scr[0:1, cs(h)])
                ds = (p * (cur - d_scr[0:1, cs(h)])).astype(BF16)
                part = dot(p.astype(BF16), do_all[i, h])
                dv = part if h == 0 else dv + part
                part = dot(ds, q_all[i, h])
                dk = part if h == 0 else dk + part
                acc_t[:, cs(h)] += dot(kt[at_j[b]], ds)
                if h == group - 1:
                    dkv[at[b], 0] += dk
                    dkv[at[b], 1] += dv

        def bwd_body(t, _):
            bwd([2 * t, 2 * t + 1])
            return 0

        lax.fori_loop(0, n // 2, bwd_body, 0)

        @pl.when(lax.rem(n, 2) == 1)
        def _():
            bwd([n - 1])

        for h in range(group):
            dq_st[i, h] = (acc_t[:, cs(h)] * sm_scale).astype(BF16).T

        @pl.when(i != y)
        def _():
            out_copies(i)[1].start()

        return 0

    lax.fori_loop(0, n_y, one_chunk, 0)
    o_out[y] = o_st[y]
    dq_out[y] = dq_st[y]

    def sib_copy(i):
        return rcopy(dkv.at[pl.ds((1 - c) * half + n_x * i, n_x)], sib_in.at[pl.ds(n_x * i, n_x)], ds_s.at[i], ds_r.at[i], sib)

    def x_copy(i, dx):
        return rcopy(dkv.at[c * half + n_x * i + x_at(dx)], x_in.at[dx, i], xs_s.at[i, dx], xs_r.at[i, dx], dev(y, x_at(dx), c))

    def y_copy(i):
        return rcopy(dkv_st.at[i], dkv_out.at[y], fy_s.at[i], fy_r.at[y], dev(i, x, c))

    slots = list(range(n_y - 1, -1, -1))
    for i in slots:
        sib_copy(i).start()
    for i in slots:
        sib_copy(i).wait_recv()

        def add(t, _):
            at = c * half + n_x * i + t
            dkv[at] = dkv[at] + sib_in[n_x * i + t]
            return 0

        lax.fori_loop(0, n_x, add, 0)
        for dx in xorder:
            x_copy(i, dx).start()
    for i in slots:
        for dx in xorder:
            x_copy(i, dx).wait_recv()
        tot = dkv[c * half + n_x * i + x]
        for dx in xorder:
            tot = tot + x_in[dx, i]
        dkv_st[i, 0] = (tot[0] * sm_scale).astype(BF16)
        dkv_st[i, 1] = tot[1].astype(BF16)

        @pl.when(i != y)
        def _():
            y_copy(i).start()

    dkv_out[y] = dkv_st[y]
    for yy in range(n_y):
        @pl.when(yy != y)
        def _():
            for k, out in enumerate((o_out, dq_out)):
                rcopy(o_st.at[yy], out.at[yy], od_s.at[k, yy], od_r.at[k, yy], sib).wait_recv()
            rcopy(dkv_st.at[yy], dkv_out.at[yy], fy_s.at[yy], fy_r.at[yy], sib).wait_recv()
            for cp in out_copies(yy):
                cp.wait_send()
            y_copy(yy).wait_send()

        sib_copy(yy).wait_send()
        for dx in xorder:
            x_copy(yy, dx).wait_send()


def solution(mesh):
    n_ctx = mesh.shape['ctx']
    seq_spec = P('dp', 'ctx', None, None)

    def local_attn(q_loc, k_loc, v_loc, do_loc):
        n_batch, chunk, q_heads, dim = q_loc.shape
        kv_heads = k_loc.shape[2]
        group = q_heads // kv_heads
        inner = n_ctx // kv_heads
        n_x = inner // 2
        n_win = WINDOW // chunk
        n_y = kv_heads
        wide = group * chunk

        def heads(x, per):
            return jnp.transpose(x[0], (1, 0, 2)).reshape(kv_heads, per, chunk, dim)

        def tokens(x):
            return jnp.transpose(x.reshape(-1, chunk, dim), (1, 0, 2))[None]

        q4, do4 = heads(q_loc, group), heads(do_loc, group)
        kv4 = jnp.concatenate([heads(k_loc, 1), heads(v_loc, 1)], axis=1)
        vm = pl.BlockSpec(memory_space=pltpu.VMEM)
        dma = pltpu.SemaphoreType.DMA
        o4, dq4, dkv4 = pl.pallas_call(
            functools.partial(attn_kernel, inner, n_win, dim ** -0.5),
            out_shape=(jax.ShapeDtypeStruct(q4.shape, BF16), jax.ShapeDtypeStruct(q4.shape, BF16),
                       jax.ShapeDtypeStruct(kv4.shape, BF16)),
            in_specs=[vm] * 3,
            out_specs=(vm,) * 3,
            scratch_shapes=[
                pltpu.VMEM(q4.shape, BF16), pltpu.VMEM(q4.shape, BF16), pltpu.VMEM((n_ctx, 2, chunk, dim), BF16),
                pltpu.VMEM((n_ctx, dim, chunk), BF16), pltpu.VMEM((n_ctx, dim, chunk), BF16),
                pltpu.VMEM((dim, wide), BF16), pltpu.VMEM((dim, wide), BF16),
                pltpu.VMEM((n_win + 1, chunk, wide), F32), pltpu.VMEM((dim, wide), F32),
                pltpu.VMEM((8, wide), F32), pltpu.VMEM((8, wide), F32),
                pltpu.VMEM((8, wide), F32), pltpu.VMEM((8, wide), F32),
                pltpu.VMEM((n_ctx, 2, chunk, dim), F32), pltpu.VMEM(q4.shape, BF16), pltpu.VMEM(q4.shape, BF16),
                pltpu.VMEM((n_ctx // 2, 2, chunk, dim), F32), pltpu.VMEM((n_x, n_y, 2, chunk, dim), F32),
                pltpu.VMEM(kv4.shape, BF16),
                dma((3,)), dma((3, n_y)), dma((3, n_y)), dma((n_y, n_x)), dma((n_y, n_x)), dma((n_y, n_x)), dma((n_y, n_x)),
                dma((2, n_y)), dma((2, n_y)), dma((n_y,)), dma((n_y,)), dma((n_y, n_x)), dma((n_y, n_x)),
                dma((n_y,)), dma((n_y,)),
            ],
            compiler_params=pltpu.CompilerParams(vmem_limit_bytes=63 * 1024 * 1024, collective_id=0, has_side_effects=True),
            name='attn_core',
        )(q4, do4, kv4)
        return tokens(o4), tokens(dq4), tokens(dkv4[:, 0]), tokens(dkv4[:, 1])

    return jax.shard_map(local_attn, mesh=mesh, in_specs=(seq_spec,) * 4, out_specs=(seq_spec,) * 4, check_vma=False)
```

```python
import functools

import jax
import jax.numpy as jnp
from jax import lax
from jax.experimental import pallas as pl
from jax.experimental.pallas import tpu as pltpu
from jax.sharding import PartitionSpec as P

WINDOW = 4096
NEG = -1e30
LOG2E = 1.4426950408889634
F32 = jnp.float32
BF16 = jnp.bfloat16


def dot(a, b):
    return jnp.dot(a, b, preferred_element_type=F32)


def fold8(x, op):
    n = x.shape[0] // 8
    acc = x[0:8]
    for t in range(1, n):
        acc = op(acc, x[8 * t:8 * t + 8])
    return acc


MESH = pl.DeviceIdType.MESH


def attn_kernel(inner, n_win, sm_scale, q_loc, do_loc, kv_loc, o_out, dq_out, dkv_out,
                q_all, do_all, kv_all, kt, vt, qt, dot_t, s_scr, acc_t, m_scr, l_scr, lse_scr, d_scr,
                dkv, o_st, dq_st, sib_in, x_in, dkv_st,
                loc_sem, in_s, in_r, ag_s, ag_r, sb_s, sb_r, od_s, od_r, ds_s, ds_r, xs_s, xs_r, fy_s, fy_r):
    n_y, group, chunk, dim = q_loc.shape
    n_kv = kv_all.shape[0]
    n_x = inner // 2
    half = n_kv // 2
    dp = lax.axis_index('dp')
    me = lax.axis_index('ctx')
    y, r = me // inner, lax.rem(me, inner)
    x, c = r // 2, lax.rem(r, 2)
    c_exp = sm_scale * LOG2E

    def dev(yy, xx, cc):
        return (dp, yy * inner + xx * 2 + cc)

    def y_at(dy):
        return lax.rem(y + dy + n_y, n_y)

    def x_at(dx):
        return lax.rem(x + dx + n_x, n_x)

    def rcopy(src, dst, s, rr, to):
        return pltpu.make_async_remote_copy(src_ref=src, dst_ref=dst, send_sem=s, recv_sem=rr, device_id=to, device_id_type=MESH)

    sib = dev(y, x, 1 - c)
    peers = [dev(y_at(d), x, c) for d in range(1, n_y)] + [dev(y, x_at(d), c) for d in range(1, n_x)] + [sib]
    barrier = pltpu.get_barrier_semaphore()
    for p in peers:
        pl.semaphore_signal(barrier, inc=1, device_id=p, device_id_type=MESH)
    pl.semaphore_wait(barrier, len(peers))

    mine = y * inner + r
    locs = [pltpu.make_async_copy(kv_loc.at[y], kv_all.at[mine], loc_sem.at[0]),
            pltpu.make_async_copy(q_loc.at[y], q_all.at[y], loc_sem.at[1]),
            pltpu.make_async_copy(do_loc.at[y], do_all.at[y], loc_sem.at[2])]
    for cp in locs:
        cp.start()
    order = [1, n_y - 1] + list(range(2, n_y - 1))
    ins = []
    for k, (src, dst, at) in enumerate(((kv_loc, kv_all, mine), (q_loc, q_all, y), (do_loc, do_all, y))):
        for d in order:
            cp = rcopy(src.at[y_at(d)], dst.at[at], in_s.at[k, d], in_r.at[k, d], dev(y_at(d), x, c))
            cp.start()
            ins.append(cp)

    def fwd_sib(slot, dx, idx):
        cp = rcopy(kv_all.at[idx], kv_all.at[idx], sb_s.at[slot, dx], sb_r.at[slot, dx], sib)
        cp.start()
        return cp

    xorder = [1, n_x - 1] + list(range(2, n_x - 1))
    ags, sbs = [], []
    for d in [0] + order:
        own = y_at(-d) * inner + r
        if d == 0:
            locs[0].wait()
        else:
            rcopy(kv_loc.at[y], kv_all.at[own], in_s.at[0, d], in_r.at[0, d], sib).wait_recv()
        for dx in xorder:
            cp = rcopy(kv_all.at[own], kv_all.at[own], ag_s.at[d, dx], ag_r.at[d, dx], dev(y, x_at(dx), c))
            cp.start()
            ags.append(cp)
        sbs.append(fwd_sib(d, 0, own))
    for d in [0] + order:
        for dx in xorder:
            idx = y_at(-d) * inner + x_at(-dx) * 2 + c
            rcopy(kv_all.at[idx], kv_all.at[idx], ag_s.at[d, dx], ag_r.at[d, dx], sib).wait_recv()
            sbs.append(fwd_sib(d, dx, idx))
    for d in [0] + order:
        for dx in [0] + xorder:
            idx = y_at(-d) * inner + x_at(-dx) * 2 + 1 - c
            rcopy(kv_all.at[idx], kv_all.at[idx], sb_s.at[d, dx], sb_r.at[d, dx], sib).wait_recv()
    for k, dst, loc in ((1, q_all, locs[1]), (2, do_all, locs[2])):
        loc.wait()
        for d in order:
            at = y_at(-d)
            rcopy(dst.at[at], dst.at[at], in_s.at[k, d], in_r.at[k, d], sib).wait_recv()
    for cp in ins + ags + sbs:
        cp.wait_send()

    def prep(j, _):
        kt[j] = kv_all[j, 0].T
        vt[j] = kv_all[j, 1].T
        dkv[j] = jnp.zeros((2, chunk, dim), F32)
        return 0

    lax.fori_loop(0, n_kv, prep, 0)
    rows = lax.broadcasted_iota(jnp.int32, (chunk, chunk), 0)
    cols = lax.broadcasted_iota(jnp.int32, (chunk, chunk), 1)

    def cs(h):
        return slice(h * chunk, (h + 1) * chunk)

    def out_copies(i):
        return [rcopy(st.at[i], out.at[y], od_s.at[k, i], od_r.at[k, y], dev(i, x, c))
                for k, (st, out) in enumerate(((o_st, o_out), (dq_st, dq_out)))]

    def sib_copy(i):
        return rcopy(dkv.at[pl.ds((1 - c) * half + n_x * i, n_x)], sib_in.at[pl.ds(n_x * i, n_x)], ds_s.at[i], ds_r.at[i], sib)

    def x_copy(i, dx):
        return rcopy(dkv.at[c * half + n_x * i + x_at(dx)], x_in.at[dx, i], xs_s.at[i, dx], xs_r.at[i, dx], dev(y, x_at(dx), c))

    def y_copy(i):
        return rcopy(dkv_st.at[i], dkv_out.at[y], fy_s.at[i], fy_r.at[y], dev(i, x, c))

    def reduce_start(i):
        sib_copy(i).wait_recv()

        def add(t, _):
            at = c * half + n_x * i + t
            dkv[at] = dkv[at] + sib_in[n_x * i + t]
            return 0

        lax.fori_loop(0, n_x, add, 0)
        for dx in xorder:
            x_copy(i, dx).start()

    def reduce_end(i):
        for dx in xorder:
            x_copy(i, dx).wait_recv()
        tot = dkv[c * half + n_x * i + x]
        for dx in xorder:
            tot = tot + x_in[dx, i]
        dkv_st[i, 0] = (tot[0] * sm_scale).astype(BF16)
        dkv_st[i, 1] = tot[1].astype(BF16)

        @pl.when(i != y)
        def _():
            y_copy(i).start()

    def one_chunk(step, _):
        i = n_y - 1 - step
        g = i * inner + r
        lo = jnp.maximum(g - n_win, 0)
        n = g - lo + 1
        for h in range(group):
            qt[:, cs(h)] = q_all[i, h].T
            dot_t[:, cs(h)] = do_all[i, h].T
        m_scr[...] = jnp.full(m_scr.shape, NEG, F32)
        l_scr[...] = jnp.zeros(l_scr.shape, F32)
        acc_t[...] = jnp.zeros(acc_t.shape, F32)

        def fwd(blocks):
            def score(h):
                return [dot(kv_all[lo + jj, 0], qt[:, cs(h)]) for jj, _ in blocks]

            nxt = score(0)
            for h in range(group):
                cur = nxt
                if h + 1 < group:
                    nxt = score(h + 1)
                m_old = m_scr[:, cs(h)]
                mx = m_old
                for (jj, keep), s in zip(blocks, cur):
                    s = s * c_exp
                    if keep is not None:
                        s = jnp.where(keep, s, NEG)
                    s_scr[jj, :, cs(h)] = s
                    mx = jnp.maximum(mx, fold8(s, jnp.maximum))
                m_new = jnp.broadcast_to(jnp.max(mx, axis=0, keepdims=True), m_old.shape)
                alpha = jnp.exp2(m_old - m_new)
                m_scr[:, cs(h)] = m_new
                l_new = l_scr[:, cs(h)] * alpha
                pv = None
                for jj, _ in blocks:
                    p = jnp.exp2(s_scr[jj, :, cs(h)] - m_new[0:1])
                    l_new = l_new + fold8(p, jnp.add)
                    part = dot(vt[lo + jj], p.astype(BF16))
                    pv = part if pv is None else pv + part
                l_scr[:, cs(h)] = l_new
                acc_t[:, cs(h)] = acc_t[:, cs(h)] * alpha[0:1] + pv

        old_edge = g >= n_win
        first = jnp.where(old_edge, 1, 0)
        n_mid = n - 1 - first

        @pl.when(old_edge)
        def _():
            fwd([(0, rows > cols), (n - 1, rows <= cols)])

        @pl.when(jnp.logical_not(old_edge))
        def _():
            fwd([(n - 1, rows <= cols)])

        def fwd_body(t, _):
            fwd([(first + 2 * t, None), (first + 2 * t + 1, None)])
            return 0

        lax.fori_loop(0, n_mid // 2, fwd_body, 0)

        @pl.when(lax.rem(n_mid, 2) == 1)
        def _():
            fwd([(first + n_mid - 1, None)])

        l_row = jnp.sum(l_scr[...], axis=0, keepdims=True)
        lse_scr[...] = jnp.broadcast_to(m_scr[0:1] + jnp.log2(l_row), lse_scr.shape)
        for h in range(group):
            o_t = (acc_t[:, cs(h)] / l_row[:, cs(h)]).astype(BF16)
            d = jnp.sum(o_t.astype(F32) * dot_t[:, cs(h)].astype(F32), axis=0, keepdims=True)
            d_scr[:, cs(h)] = jnp.broadcast_to(d, (8, chunk))
            o_st[i, h] = o_t.T
        acc_t[...] = jnp.zeros(acc_t.shape, F32)

        @pl.when(i != y)
        def _():
            out_copies(i)[0].start()

        @pl.when(step > 0)
        def _():
            reduce_start(i + 1)

        def bwd(jjs):
            units = [(b, h) for b in range(len(jjs)) for h in range(group)]
            at_j = [lo + jj for jj in jjs]
            at = [lax.rem(j, 2) * half + j // 2 for j in at_j]

            def grad_p(b, h):
                return dot(kv_all[at_j[b], 1], dot_t[:, cs(h)])

            nxt = grad_p(*units[0])
            dk = dv = None
            for k, (b, h) in enumerate(units):
                cur = nxt
                if k + 1 < len(units):
                    nxt = grad_p(*units[k + 1])
                p = jnp.exp2(s_scr[jjs[b], :, cs(h)] - lse_scr[0:1, cs(h)])
                ds = (p * (cur - d_scr[0:1, cs(h)])).astype(BF16)
                part = dot(p.astype(BF16), do_all[i, h])
                dv = part if h == 0 else dv + part
                part = dot(ds, q_all[i, h])
                dk = part if h == 0 else dk + part
                acc_t[:, cs(h)] += dot(kt[at_j[b]], ds)
                if h == group - 1:
                    dkv[at[b], 0] += dk
                    dkv[at[b], 1] += dv

        def bwd_body(t, _):
            bwd([2 * t, 2 * t + 1])
            return 0

        lax.fori_loop(0, n // 2, bwd_body, 0)

        @pl.when(lax.rem(n, 2) == 1)
        def _():
            bwd([n - 1])

        for h in range(group):
            dq_st[i, h] = (acc_t[:, cs(h)] * sm_scale).astype(BF16).T

        @pl.when(i != y)
        def _():
            out_copies(i)[1].start()

        sib_copy(i).start()

        @pl.when(step > 0)
        def _():
            reduce_end(i + 1)

        return 0

    lax.fori_loop(0, n_y, one_chunk, 0)
    reduce_start(0)
    o_out[y] = o_st[y]
    dq_out[y] = dq_st[y]
    reduce_end(0)

    dkv_out[y] = dkv_st[y]
    for yy in range(n_y):
        @pl.when(yy != y)
        def _():
            for k, out in enumerate((o_out, dq_out)):
                rcopy(o_st.at[yy], out.at[yy], od_s.at[k, yy], od_r.at[k, yy], sib).wait_recv()
            rcopy(dkv_st.at[yy], dkv_out.at[yy], fy_s.at[yy], fy_r.at[yy], sib).wait_recv()
            for cp in out_copies(yy):
                cp.wait_send()
            y_copy(yy).wait_send()

        sib_copy(yy).wait_send()
        for dx in xorder:
            x_copy(yy, dx).wait_send()


def solution(mesh):
    n_ctx = mesh.shape['ctx']
    seq_spec = P('dp', 'ctx', None, None)

    def local_attn(q_loc, k_loc, v_loc, do_loc):
        n_batch, chunk, q_heads, dim = q_loc.shape
        kv_heads = k_loc.shape[2]
        group = q_heads // kv_heads
        inner = n_ctx // kv_heads
        n_x = inner // 2
        n_win = WINDOW // chunk
        n_y = kv_heads
        wide = group * chunk

        def heads(x, per):
            return jnp.transpose(x[0], (1, 0, 2)).reshape(kv_heads, per, chunk, dim)

        def tokens(x):
            return jnp.transpose(x.reshape(-1, chunk, dim), (1, 0, 2))[None]

        q4, do4 = heads(q_loc, group), heads(do_loc, group)
        kv4 = jnp.concatenate([heads(k_loc, 1), heads(v_loc, 1)], axis=1)
        vm = pl.BlockSpec(memory_space=pltpu.VMEM)
        dma = pltpu.SemaphoreType.DMA
        o4, dq4, dkv4 = pl.pallas_call(
            functools.partial(attn_kernel, inner, n_win, dim ** -0.5),
            out_shape=(jax.ShapeDtypeStruct(q4.shape, BF16), jax.ShapeDtypeStruct(q4.shape, BF16),
                       jax.ShapeDtypeStruct(kv4.shape, BF16)),
            in_specs=[vm] * 3,
            out_specs=(vm,) * 3,
            scratch_shapes=[
                pltpu.VMEM(q4.shape, BF16), pltpu.VMEM(q4.shape, BF16), pltpu.VMEM((n_ctx, 2, chunk, dim), BF16),
                pltpu.VMEM((n_ctx, dim, chunk), BF16), pltpu.VMEM((n_ctx, dim, chunk), BF16),
                pltpu.VMEM((dim, wide), BF16), pltpu.VMEM((dim, wide), BF16),
                pltpu.VMEM((n_win + 1, chunk, wide), F32), pltpu.VMEM((dim, wide), F32),
                pltpu.VMEM((8, wide), F32), pltpu.VMEM((8, wide), F32),
                pltpu.VMEM((8, wide), F32), pltpu.VMEM((8, wide), F32),
                pltpu.VMEM((n_ctx, 2, chunk, dim), F32), pltpu.VMEM(q4.shape, BF16), pltpu.VMEM(q4.shape, BF16),
                pltpu.VMEM((n_ctx // 2, 2, chunk, dim), F32), pltpu.VMEM((n_x, n_y, 2, chunk, dim), F32),
                pltpu.VMEM(kv4.shape, BF16),
                dma((3,)), dma((3, n_y)), dma((3, n_y)), dma((n_y, n_x)), dma((n_y, n_x)), dma((n_y, n_x)), dma((n_y, n_x)),
                dma((2, n_y)), dma((2, n_y)), dma((n_y,)), dma((n_y,)), dma((n_y, n_x)), dma((n_y, n_x)),
                dma((n_y,)), dma((n_y,)),
            ],
            compiler_params=pltpu.CompilerParams(vmem_limit_bytes=63 * 1024 * 1024, collective_id=0, has_side_effects=True),
            name='attn_core',
        )(q4, do4, kv4)
        return tokens(o4), tokens(dq4), tokens(dkv4[:, 0]), tokens(dkv4[:, 1])

    return jax.shard_map(local_attn, mesh=mesh, in_specs=(seq_spec,) * 4, out_specs=(seq_spec,) * 4, check_vma=False)
```

```python
import functools

import jax
import jax.numpy as jnp
from jax import lax
from jax.experimental import pallas as pl
from jax.experimental.pallas import tpu as pltpu
from jax.sharding import PartitionSpec as P

WINDOW = 4096
NEG = -1e30
LOG2E = 1.4426950408889634
F32 = jnp.float32
BF16 = jnp.bfloat16


def dot(a, b):
    return jnp.dot(a, b, preferred_element_type=F32)


def fold8(x, op):
    n = x.shape[0] // 8
    acc = x[0:8]
    for t in range(1, n):
        acc = op(acc, x[8 * t:8 * t + 8])
    return acc


MESH = pl.DeviceIdType.MESH


def attn_kernel(inner, n_win, sm_scale, q_loc, do_loc, kv_loc, o_out, dq_out, dkv_out,
                q_all, do_all, kv_all, kt, vt, qt, dot_t, s_scr, acc_t, m_scr, l_scr, lse_scr, d_scr,
                p_a, s_a, p_b, s_b, dkv, o_st, dq_st, sib_in, x_in, dkv_st,
                loc_sem, in_s, in_r, ag_s, ag_r, sb_s, sb_r, od_s, od_r, ds_s, ds_r, xs_s, xs_r, fy_s, fy_r):
    n_y, group, chunk, dim = q_loc.shape
    n_kv = kv_all.shape[0]
    n_x = inner // 2
    half = n_kv // 2
    top = n_y - 1
    dp = lax.axis_index('dp')
    me = lax.axis_index('ctx')
    y, r = me // inner, lax.rem(me, inner)
    x, c = r // 2, lax.rem(r, 2)
    c_exp = sm_scale * LOG2E

    def dev(yy, xx, cc):
        return (dp, yy * inner + xx * 2 + cc)

    def y_at(dy):
        return lax.rem(y + dy + n_y, n_y)

    def x_at(dx):
        return lax.rem(x + dx + n_x, n_x)

    def rcopy(src, dst, s, rr, to):
        return pltpu.make_async_remote_copy(src_ref=src, dst_ref=dst, send_sem=s, recv_sem=rr, device_id=to, device_id_type=MESH)

    sib = dev(y, x, 1 - c)
    peers = [dev(y_at(d), x, c) for d in range(1, n_y)] + [dev(y, x_at(d), c) for d in range(1, n_x)] + [sib]
    barrier = pltpu.get_barrier_semaphore()
    for p in peers:
        pl.semaphore_signal(barrier, inc=1, device_id=p, device_id_type=MESH)
    pl.semaphore_wait(barrier, len(peers))

    yorder = [1, n_y - 1] + list(range(2, n_y - 1))
    xorder = [1, n_x - 1] + list(range(2, n_x - 1))
    mine = y * inner + r
    locs = [pltpu.make_async_copy(kv_loc.at[y], kv_all.at[mine], loc_sem.at[0]),
            pltpu.make_async_copy(q_loc.at[y], q_all.at[y], loc_sem.at[1]),
            pltpu.make_async_copy(do_loc.at[y], do_all.at[y], loc_sem.at[2])]
    for cp in locs:
        cp.start()

    def kv_copy(d):
        return rcopy(kv_loc.at[y_at(d)], kv_all.at[mine], in_s.at[0, d], in_r.at[0, d], dev(y_at(d), x, c))

    def qdo_copies(d):
        return [rcopy(src.at[y_at(d)], dst.at[y], in_s.at[k, d], in_r.at[k, d], dev(y_at(d), x, c))
                for k, src, dst in ((1, q_loc, q_all), (2, do_loc, do_all))]

    def send_qdo():
        for d in yorder:
            for cp in qdo_copies(d):
                cp.start()

    def wait_qdo(s):
        @pl.when(s != y)
        def _():
            d = y_at(-s)
            for k, dst in ((1, q_all), (2, do_all)):
                rcopy(dst.at[s], dst.at[s], in_s.at[k, d], in_r.at[k, d], sib).wait_recv()

    def ag_copy(s, dx):
        idx = s * inner + r
        return rcopy(kv_all.at[idx], kv_all.at[idx], ag_s.at[s, dx], ag_r.at[s, dx], dev(y, x_at(dx), c))

    def sb_copy(s, dx):
        idx = s * inner + x_at(-dx) * 2 + c
        return rcopy(kv_all.at[idx], kv_all.at[idx], sb_s.at[s, dx], sb_r.at[s, dx], sib)

    for d in yorder:
        kv_copy(d).start()

    @pl.when(y == top)
    def _():
        send_qdo()

    slots = list(range(top, -1, -1))
    for s in slots:
        idx = s * inner + r

        @pl.when(s == y)
        def _():
            locs[0].wait()

        @pl.when(s != y)
        def _():
            d = y_at(-s)
            rcopy(kv_all.at[idx], kv_all.at[idx], in_s.at[0, d], in_r.at[0, d], sib).wait_recv()

        for dx in xorder:
            ag_copy(s, dx).start()
        sb_copy(s, 0).start()

    def ready(s):
        for dx in xorder:
            idx = s * inner + x_at(-dx) * 2 + c
            rcopy(kv_all.at[idx], kv_all.at[idx], ag_s.at[s, dx], ag_r.at[s, dx], sib).wait_recv()
            sb_copy(s, dx).start()
        for dx in [0] + xorder:
            idx = s * inner + x_at(-dx) * 2 + 1 - c
            rcopy(kv_all.at[idx], kv_all.at[idx], sb_s.at[s, dx], sb_r.at[s, dx], sib).wait_recv()

        def prep(t, _):
            j = s * inner + t
            kt[j] = kv_all[j, 0].T
            vt[j] = kv_all[j, 1].T
            dkv[lax.rem(j, 2) * half + j // 2] = jnp.zeros((2, chunk, dim), F32)
            return 0

        lax.fori_loop(0, inner, prep, 0)

    ready(top)

    @pl.when(r == 0)
    def _():
        ready(top - 1)

    locs[1].wait()
    locs[2].wait()
    wait_qdo(top)

    @pl.when(y != top)
    def _():
        send_qdo()

    need_1 = (r + 1) // 2
    need_2 = (r + inner + 1) // 2
    diff = lax.broadcasted_iota(jnp.int32, (chunk, chunk), 0) - lax.broadcasted_iota(jnp.int32, (chunk, chunk), 1)

    def cs(h):
        return slice(h * chunk, (h + 1) * chunk)

    def out_copies(i):
        return [rcopy(st.at[i], out.at[y], od_s.at[k, i], od_r.at[k, y], dev(i, x, c))
                for k, (st, out) in enumerate(((o_st, o_out), (dq_st, dq_out)))]

    def sib_copy(i):
        return rcopy(dkv.at[pl.ds((1 - c) * half + n_x * i, n_x)], sib_in.at[pl.ds(n_x * i, n_x)], ds_s.at[i], ds_r.at[i], sib)

    def x_copy(i, dx):
        return rcopy(dkv.at[c * half + n_x * i + x_at(dx)], x_in.at[dx, i], xs_s.at[i, dx], xs_r.at[i, dx], dev(y, x_at(dx), c))

    def y_copy(i):
        return rcopy(dkv_st.at[i], dkv_out.at[y], fy_s.at[i], fy_r.at[y], dev(i, x, c))

    def reduce_start(i):
        sib_copy(i).wait_recv()

        def add(t, _):
            at = c * half + n_x * i + t
            dkv[at] = dkv[at] + sib_in[n_x * i + t]
            return 0

        lax.fori_loop(0, n_x, add, 0)
        for dx in xorder:
            x_copy(i, dx).start()

    def reduce_end(i):
        for dx in xorder:
            x_copy(i, dx).wait_recv()
        tot = dkv[c * half + n_x * i + x]
        for dx in xorder:
            tot = tot + x_in[dx, i]
        dkv_st[i, 0] = (tot[0] * sm_scale).astype(BF16)
        dkv_st[i, 1] = tot[1].astype(BF16)

        @pl.when(i != y)
        def _():
            y_copy(i).start()

    def one_chunk(step, _):
        i = top - step
        g = i * inner + r
        n = jnp.maximum(jnp.minimum(g, n_win) + 1, 2)
        for h in range(group):
            qt[:, cs(h)] = q_all[i, h].T
            dot_t[:, cs(h)] = do_all[i, h].T
        m_scr[...] = jnp.full(m_scr.shape, NEG, F32)
        l_scr[...] = jnp.zeros(l_scr.shape, F32)
        lse_scr[...] = jnp.full(lse_scr.shape, NEG, F32)
        acc_t[...] = jnp.zeros(acc_t.shape, F32)

        def key_of(k):
            return jnp.maximum(g - k, 0)

        def score(h, blocks):
            return [dot(kv_all[key_of(k), 0], qt[:, cs(h)]) for k, _ in blocks]

        def keep_score(h, blocks, scores):
            mx = m_scr[:, cs(h)]
            for (k, keep), s in zip(blocks, scores):
                s = s * c_exp
                if keep is not None:
                    s = jnp.where(keep, s, NEG)
                s_scr[k, :, cs(h)] = s
                mx = jnp.maximum(mx, fold8(s, jnp.maximum))
            m_scr[:, cs(h)] = mx

        def softmax_pv(h, blocks, m_new):
            m_old = lse_scr[:, cs(h)]
            alpha = jnp.exp2(m_old - m_new)
            lse_scr[:, cs(h)] = m_new
            l_new = l_scr[:, cs(h)] * alpha
            pv = None
            for k, _ in blocks:
                p = jnp.exp2(s_scr[k, :, cs(h)] - m_new[0:1])
                l_new = l_new + fold8(p, jnp.add)
                part = dot(vt[key_of(k)], p.astype(BF16))
                pv = part if pv is None else pv + part
            l_scr[:, cs(h)] = l_new
            acc_t[:, cs(h)] = acc_t[:, cs(h)] * alpha[0:1] + pv

        def row_max(h):
            m = m_scr[:, cs(h)]
            return jnp.broadcast_to(jnp.max(m, axis=0, keepdims=True), m.shape)

        def fwd(new, old):
            if old:
                m_new = [row_max(h) for h in range(group)]
            for h in range(group):
                if new:
                    scores = score(h, new)
                if old:
                    softmax_pv(h, old, m_new[h])
                if new:
                    keep_score(h, new, scores)

        def pair(p):
            return [(2 * p, None), (2 * p + 1, None)]

        n_pair = n // 2
        odd = lax.rem(n, 2) == 1
        last = [(n - 1, diff > jnp.where(g >= n_win, 0, -2 * chunk))]
        fwd([(0, diff <= 0), (1, diff < jnp.where(g > 0, 2 * chunk, -2 * chunk))], None)

        def fwd_body(p, _):
            @pl.when((step == 0) & (p == need_1))
            def _():
                ready(top - 1)

            @pl.when((step == 0) & (p == need_2))
            def _():
                ready(top - 2)

            fwd(pair(p), pair(p - 1))
            return 0

        lax.fori_loop(1, n_pair, fwd_body, 0)

        @pl.when(odd)
        def _():
            @pl.when((step == 0) & (n_pair == need_2))
            def _():
                ready(top - 2)

            fwd(last, pair(n_pair - 1))
            fwd(None, last)

        @pl.when(jnp.logical_not(odd))
        def _():
            fwd(None, pair(n_pair - 1))

        l_row = jnp.sum(l_scr[...], axis=0, keepdims=True)
        lse_scr[...] = lse_scr[...] + jnp.log2(l_row)
        for h in range(group):
            o_t = (acc_t[:, cs(h)] / l_row[:, cs(h)]).astype(BF16)
            d = jnp.sum(o_t.astype(F32) * dot_t[:, cs(h)].astype(F32), axis=0, keepdims=True)
            d_scr[:, cs(h)] = jnp.broadcast_to(d, (8, chunk))
            o_st[i, h] = o_t.T
        acc_t[...] = jnp.zeros(acc_t.shape, F32)

        @pl.when(i != y)
        def _():
            out_copies(i)[0].start()

        @pl.when(step > 0)
        def _():
            reduce_start(i + 1)

        buf_a, buf_b = (p_a, s_a), (p_b, s_b)

        def grad(k1, buf1, k2, buf2):
            if k1 is not None:
                j1 = key_of(k1)
            if k2 is not None:
                j2 = key_of(k2)
                at = lax.rem(j2, 2) * half + j2 // 2
                pb, sb = buf2
            for h in range(group):
                if k1 is not None:
                    dp_t = dot(kv_all[j1, 1], dot_t[:, cs(h)])
                if k2 is not None:
                    if h == 0:
                        dkv[at, 1] += dot(pb[...], do_all[i].reshape(group * chunk, dim))
                    elif h == 1:
                        dkv[at, 0] += dot(sb[...], q_all[i].reshape(group * chunk, dim))
                    for e in range(group):
                        if min(2 + e // (group // 2), group - 1) == h:
                            acc_t[:, cs(e)] += dot(kt[j2], sb[:, cs(e)])
                if k1 is not None:
                    p = jnp.exp2(s_scr[k1, :, cs(h)] - lse_scr[0:1, cs(h)])
                    buf1[0][:, cs(h)] = p.astype(BF16)
                    buf1[1][:, cs(h)] = (p * (dp_t - d_scr[0:1, cs(h)])).astype(BF16)

        grad(0, buf_a, None, None)

        def bwd_body(t, _):
            grad(2 * t + 1, buf_b, 2 * t, buf_a)
            grad(2 * t + 2, buf_a, 2 * t + 1, buf_b)
            return 0

        lax.fori_loop(0, (n - 1) // 2, bwd_body, 0)

        @pl.when(odd)
        def _():
            grad(None, None, n - 1, buf_a)

        @pl.when(jnp.logical_not(odd))
        def _():
            grad(n - 1, buf_b, n - 2, buf_a)
            grad(None, None, n - 1, buf_b)

        for h in range(group):
            dq_st[i, h] = (acc_t[:, cs(h)] * sm_scale).astype(BF16).T

        @pl.when(i != y)
        def _():
            out_copies(i)[1].start()

        sib_copy(i).start()

        @pl.when(step == 0)
        def _():
            for s in slots[3:]:
                ready(s)
            for s in slots[1:]:
                wait_qdo(s)

        @pl.when(step > 0)
        def _():
            reduce_end(i + 1)

        return 0

    lax.fori_loop(0, n_y, one_chunk, 0)
    reduce_start(0)
    o_out[y] = o_st[y]
    dq_out[y] = dq_st[y]
    for d in yorder:
        for cp in [kv_copy(d)] + qdo_copies(d):
            cp.wait_send()
    for s in slots:
        sb_copy(s, 0).wait_send()
        for dx in xorder:
            ag_copy(s, dx).wait_send()
            sb_copy(s, dx).wait_send()
    reduce_end(0)
    dkv_out[y] = dkv_st[y]
    for yy in range(n_y):
        @pl.when(yy != y)
        def _():
            for k, out in enumerate((o_out, dq_out)):
                rcopy(o_st.at[yy], out.at[yy], od_s.at[k, yy], od_r.at[k, yy], sib).wait_recv()
            rcopy(dkv_st.at[yy], dkv_out.at[yy], fy_s.at[yy], fy_r.at[yy], sib).wait_recv()
            for cp in out_copies(yy):
                cp.wait_send()
            y_copy(yy).wait_send()

        sib_copy(yy).wait_send()
        for dx in xorder:
            x_copy(yy, dx).wait_send()


def solution(mesh):
    n_ctx = mesh.shape['ctx']
    seq_spec = P('dp', 'ctx', None, None)

    def local_attn(q_loc, k_loc, v_loc, do_loc):
        n_batch, chunk, q_heads, dim = q_loc.shape
        kv_heads = k_loc.shape[2]
        group = q_heads // kv_heads
        inner = n_ctx // kv_heads
        n_x = inner // 2
        n_win = WINDOW // chunk
        n_y = kv_heads
        wide = group * chunk

        def heads(x, per):
            return jnp.transpose(x[0], (1, 0, 2)).reshape(kv_heads, per, chunk, dim)

        def tokens(x):
            return jnp.transpose(x.reshape(-1, chunk, dim), (1, 0, 2))[None]

        q4, do4 = heads(q_loc, group), heads(do_loc, group)
        kv4 = jnp.concatenate([heads(k_loc, 1), heads(v_loc, 1)], axis=1)
        vm = pl.BlockSpec(memory_space=pltpu.VMEM)
        dma = pltpu.SemaphoreType.DMA
        o4, dq4, dkv4 = pl.pallas_call(
            functools.partial(attn_kernel, inner, n_win, dim ** -0.5),
            out_shape=(jax.ShapeDtypeStruct(q4.shape, BF16), jax.ShapeDtypeStruct(q4.shape, BF16),
                       jax.ShapeDtypeStruct(kv4.shape, BF16)),
            in_specs=[vm] * 3,
            out_specs=(vm,) * 3,
            scratch_shapes=[
                pltpu.VMEM(q4.shape, BF16), pltpu.VMEM(q4.shape, BF16), pltpu.VMEM((n_ctx, 2, chunk, dim), BF16),
                pltpu.VMEM((n_ctx, dim, chunk), BF16), pltpu.VMEM((n_ctx, dim, chunk), BF16),
                pltpu.VMEM((dim, wide), BF16), pltpu.VMEM((dim, wide), BF16),
                pltpu.VMEM((n_win + 1, chunk, wide), F32), pltpu.VMEM((dim, wide), F32),
                pltpu.VMEM((8, wide), F32), pltpu.VMEM((8, wide), F32),
                pltpu.VMEM((8, wide), F32), pltpu.VMEM((8, wide), F32),
                pltpu.VMEM((chunk, wide), BF16), pltpu.VMEM((chunk, wide), BF16),
                pltpu.VMEM((chunk, wide), BF16), pltpu.VMEM((chunk, wide), BF16),
                pltpu.VMEM((n_ctx, 2, chunk, dim), F32), pltpu.VMEM(q4.shape, BF16), pltpu.VMEM(q4.shape, BF16),
                pltpu.VMEM((n_ctx // 2, 2, chunk, dim), F32), pltpu.VMEM((n_x, n_y, 2, chunk, dim), F32),
                pltpu.VMEM(kv4.shape, BF16),
                dma((3,)), dma((3, n_y)), dma((3, n_y)), dma((n_y, n_x)), dma((n_y, n_x)), dma((n_y, n_x)), dma((n_y, n_x)),
                dma((2, n_y)), dma((2, n_y)), dma((n_y,)), dma((n_y,)), dma((n_y, n_x)), dma((n_y, n_x)),
                dma((n_y,)), dma((n_y,)),
            ],
            compiler_params=pltpu.CompilerParams(vmem_limit_bytes=63 * 1024 * 1024, collective_id=0, has_side_effects=True),
            name='attn_core',
        )(q4, do4, kv4)
        return tokens(o4), tokens(dq4), tokens(dkv4[:, 0]), tokens(dkv4[:, 1])

    return jax.shard_map(local_attn, mesh=mesh, in_specs=(seq_spec,) * 4, out_specs=(seq_spec,) * 4, check_vma=False)
```

```python
import functools

import jax
import jax.numpy as jnp
from jax import lax
from jax.experimental import pallas as pl
from jax.experimental.pallas import tpu as pltpu
from jax.sharding import PartitionSpec as P

WINDOW = 4096
NEG = -1e30
LOG2E = 1.4426950408889634
F32 = jnp.float32
BF16 = jnp.bfloat16


def dot(a, b):
    return jnp.dot(a, b, preferred_element_type=F32)


def fold8(x, op):
    n = x.shape[0] // 8
    acc = x[0:8]
    for t in range(1, n):
        acc = op(acc, x[8 * t:8 * t + 8])
    return acc


MESH = pl.DeviceIdType.MESH


def attn_kernel(inner, n_win, sm_scale, q_loc, do_loc, kv_loc, o_out, dq_out, dkv_out,
                q_all, do_all, kv_all, kt, vt, qt, dot_t, s_scr, acc_t, m_scr, l_scr, lse_scr, d_scr,
                p_a, s_a, p_b, s_b, dkv, o_st, dq_st, sib_in, x_in, dkv_st,
                loc_sem, in_s, in_r, ag_s, ag_r, sb_s, sb_r, od_s, od_r, ds_s, ds_r, xs_s, xs_r, fy_s, fy_r):
    n_y, group, chunk, dim = q_loc.shape
    n_kv = kv_all.shape[0]
    n_x = inner // 2
    half = n_kv // 2
    top = n_y - 1
    dp = lax.axis_index('dp')
    me = lax.axis_index('ctx')
    y, r = me // inner, lax.rem(me, inner)
    x, c = r // 2, lax.rem(r, 2)
    c_exp = sm_scale * LOG2E

    def dev(yy, xx, cc):
        return (dp, yy * inner + xx * 2 + cc)

    def y_at(dy):
        return lax.rem(y + dy + n_y, n_y)

    def x_at(dx):
        return lax.rem(x + dx + n_x, n_x)

    def rcopy(src, dst, s, rr, to):
        return pltpu.make_async_remote_copy(src_ref=src, dst_ref=dst, send_sem=s, recv_sem=rr, device_id=to, device_id_type=MESH)

    sib = dev(y, x, 1 - c)
    peers = [dev(y_at(d), x, c) for d in range(1, n_y)] + [dev(y, x_at(d), c) for d in range(1, n_x)] + [sib]
    barrier = pltpu.get_barrier_semaphore()
    for p in peers:
        pl.semaphore_signal(barrier, inc=1, device_id=p, device_id_type=MESH)
    pl.semaphore_wait(barrier, len(peers))

    yorder = [1, n_y - 1] + list(range(2, n_y - 1))
    xorder = [1, n_x - 1] + list(range(2, n_x - 1))
    mine = y * inner + r
    locs = [pltpu.make_async_copy(kv_loc.at[y], kv_all.at[mine], loc_sem.at[0]),
            pltpu.make_async_copy(q_loc.at[y], q_all.at[y], loc_sem.at[1]),
            pltpu.make_async_copy(do_loc.at[y], do_all.at[y], loc_sem.at[2])]
    for cp in locs:
        cp.start()

    def kv_copy(d):
        return rcopy(kv_loc.at[y_at(d)], kv_all.at[mine], in_s.at[0, d], in_r.at[0, d], dev(y_at(d), x, c))

    qdo = ((1, q_loc, q_all), (2, do_loc, do_all))

    def qdo_copy(which, d):
        k, src, dst = which
        return rcopy(src.at[y_at(d)], dst.at[y], in_s.at[k, d], in_r.at[k, d], dev(y_at(d), x, c))

    def send_qdo():
        for which in qdo:
            for d in yorder:
                qdo_copy(which, d).start()

    def wait_in(which, s):
        k, _, dst = which

        @pl.when(s != y)
        def _():
            d = y_at(-s)
            rcopy(dst.at[s], dst.at[s], in_s.at[k, d], in_r.at[k, d], sib).wait_recv()

    def ag_copy(s, dx):
        idx = s * inner + r
        return rcopy(kv_all.at[idx], kv_all.at[idx], ag_s.at[s, dx], ag_r.at[s, dx], dev(y, x_at(dx), c))

    def sb_copy(s, dx):
        idx = s * inner + x_at(-dx) * 2 + c
        return rcopy(kv_all.at[idx], kv_all.at[idx], sb_s.at[s, dx], sb_r.at[s, dx], sib)

    for d in yorder:
        kv_copy(d).start()

    @pl.when(y == top)
    def _():
        send_qdo()

    slots = list(range(top, -1, -1))
    for s in slots:
        idx = s * inner + r

        @pl.when(s == y)
        def _():
            locs[0].wait()

        @pl.when(s != y)
        def _():
            d = y_at(-s)
            rcopy(kv_all.at[idx], kv_all.at[idx], in_s.at[0, d], in_r.at[0, d], sib).wait_recv()

        for dx in xorder:
            ag_copy(s, dx).start()
        sb_copy(s, 0).start()

    def ready(s):
        for dx in xorder:
            idx = s * inner + x_at(-dx) * 2 + c
            rcopy(kv_all.at[idx], kv_all.at[idx], ag_s.at[s, dx], ag_r.at[s, dx], sib).wait_recv()
            sb_copy(s, dx).start()
        for dx in [0] + xorder:
            idx = s * inner + x_at(-dx) * 2 + 1 - c
            rcopy(kv_all.at[idx], kv_all.at[idx], sb_s.at[s, dx], sb_r.at[s, dx], sib).wait_recv()

        def prep(t, _):
            j = s * inner + t
            kt[j] = kv_all[j, 0].T
            vt[j] = kv_all[j, 1].T
            dkv[lax.rem(j, 2) * half + j // 2] = jnp.zeros((2, chunk, dim), F32)
            return 0

        lax.fori_loop(0, inner, prep, 0)

    @pl.when(y != top)
    def _():
        send_qdo()

    ready(top)

    @pl.when(r == 0)
    def _():
        ready(top - 1)

    locs[1].wait()
    locs[2].wait()
    wait_in(qdo[0], top)

    need_1 = (r + 1) // 2
    need_2 = (r + inner + 1) // 2
    diff = lax.broadcasted_iota(jnp.int32, (chunk, chunk), 0) - lax.broadcasted_iota(jnp.int32, (chunk, chunk), 1)

    def cs(h):
        return slice(h * chunk, (h + 1) * chunk)

    def out_copies(i):
        return [rcopy(st.at[i], out.at[y], od_s.at[k, i], od_r.at[k, y], dev(i, x, c))
                for k, (st, out) in enumerate(((o_st, o_out), (dq_st, dq_out)))]

    def sib_copy(i):
        return rcopy(dkv.at[pl.ds((1 - c) * half + n_x * i, n_x)], sib_in.at[pl.ds(n_x * i, n_x)], ds_s.at[i], ds_r.at[i], sib)

    def x_copy(i, dx):
        return rcopy(dkv.at[c * half + n_x * i + x_at(dx)], x_in.at[dx, i], xs_s.at[i, dx], xs_r.at[i, dx], dev(y, x_at(dx), c))

    def y_copy(i):
        return rcopy(dkv_st.at[i], dkv_out.at[y], fy_s.at[i], fy_r.at[y], dev(i, x, c))

    def reduce_start(i):
        sib_copy(i).wait_recv()

        def add(t, _):
            at = c * half + n_x * i + t
            dkv[at] = dkv[at] + sib_in[n_x * i + t]
            return 0

        lax.fori_loop(0, n_x, add, 0)
        for dx in xorder:
            x_copy(i, dx).start()

    def reduce_end(i):
        for dx in xorder:
            x_copy(i, dx).wait_recv()
        tot = dkv[c * half + n_x * i + x]
        for dx in xorder:
            tot = tot + x_in[dx, i]
        dkv_st[i, 0] = (tot[0] * sm_scale).astype(BF16)
        dkv_st[i, 1] = tot[1].astype(BF16)

        @pl.when(i != y)
        def _():
            y_copy(i).start()

    def one_chunk(step, _):
        i = top - step
        g = i * inner + r
        n = jnp.maximum(jnp.minimum(g, n_win) + 1, 2)
        for h in range(group):
            qt[:, cs(h)] = q_all[i, h].T
        m_scr[...] = jnp.full(m_scr.shape, NEG, F32)
        l_scr[...] = jnp.zeros(l_scr.shape, F32)
        lse_scr[...] = jnp.full(lse_scr.shape, NEG, F32)
        acc_t[...] = jnp.zeros(acc_t.shape, F32)

        def key_of(k):
            return jnp.maximum(g - k, 0)

        def score(h, blocks):
            return [dot(kv_all[key_of(k), 0], qt[:, cs(h)]) for k, _ in blocks]

        def keep_score(h, blocks, scores):
            mx = m_scr[:, cs(h)]
            for (k, keep), s in zip(blocks, scores):
                s = s * c_exp
                if keep is not None:
                    s = jnp.where(keep, s, NEG)
                s_scr[k, :, cs(h)] = s
                mx = jnp.maximum(mx, fold8(s, jnp.maximum))
            m_scr[:, cs(h)] = mx

        def softmax_pv(h, blocks, m_new):
            m_old = lse_scr[:, cs(h)]
            alpha = jnp.exp2(m_old - m_new)
            lse_scr[:, cs(h)] = m_new
            l_new = l_scr[:, cs(h)] * alpha
            pv = None
            for k, _ in blocks:
                p = jnp.exp2(s_scr[k, :, cs(h)] - m_new[0:1])
                l_new = l_new + fold8(p, jnp.add)
                part = dot(vt[key_of(k)], p.astype(BF16))
                pv = part if pv is None else pv + part
            l_scr[:, cs(h)] = l_new
            acc_t[:, cs(h)] = acc_t[:, cs(h)] * alpha[0:1] + pv

        def row_max(h):
            m = m_scr[:, cs(h)]
            return jnp.broadcast_to(jnp.max(m, axis=0, keepdims=True), m.shape)

        def fwd(new, old):
            if old:
                m_new = [row_max(h) for h in range(group)]
            for h in range(group):
                if new:
                    scores = score(h, new)
                if old:
                    softmax_pv(h, old, m_new[h])
                if new:
                    keep_score(h, new, scores)

        def pair(p):
            return [(2 * p, None), (2 * p + 1, None)]

        n_pair = n // 2
        odd = lax.rem(n, 2) == 1
        last = [(n - 1, diff > jnp.where(g >= n_win, 0, -2 * chunk))]
        fwd([(0, diff <= 0), (1, diff < jnp.where(g > 0, 2 * chunk, -2 * chunk))], None)

        def fwd_body(p, _):
            @pl.when((step == 0) & (p == need_1))
            def _():
                ready(top - 1)

            @pl.when((step == 0) & (p == need_2))
            def _():
                ready(top - 2)

            fwd(pair(p), pair(p - 1))
            return 0

        lax.fori_loop(1, n_pair, fwd_body, 0)

        @pl.when(odd)
        def _():
            @pl.when((step == 0) & (n_pair == need_2))
            def _():
                ready(top - 2)

            fwd(last, pair(n_pair - 1))
            fwd(None, last)

        @pl.when(jnp.logical_not(odd))
        def _():
            fwd(None, pair(n_pair - 1))

        @pl.when(step == 0)
        def _():
            wait_in(qdo[1], top)

        for h in range(group):
            dot_t[:, cs(h)] = do_all[i, h].T
        l_row = jnp.sum(l_scr[...], axis=0, keepdims=True)
        lse_scr[...] = lse_scr[...] + jnp.log2(l_row)
        for h in range(group):
            o_t = (acc_t[:, cs(h)] / l_row[:, cs(h)]).astype(BF16)
            d = jnp.sum(o_t.astype(F32) * dot_t[:, cs(h)].astype(F32), axis=0, keepdims=True)
            d_scr[:, cs(h)] = jnp.broadcast_to(d, (8, chunk))
            o_st[i, h] = o_t.T
        acc_t[...] = jnp.zeros(acc_t.shape, F32)

        @pl.when(i != y)
        def _():
            out_copies(i)[0].start()

        buf_a, buf_b = (p_a, s_a), (p_b, s_b)

        def grad(k1, buf1, k2, buf2):
            if k1 is not None:
                j1 = key_of(k1)
            if k2 is not None:
                j2 = key_of(k2)
                at = lax.rem(j2, 2) * half + j2 // 2
                pb, sb = buf2
            for h in range(group):
                if k1 is not None:
                    dp_t = dot(kv_all[j1, 1], dot_t[:, cs(h)])
                if k2 is not None:
                    if h == 0:
                        dkv[at, 1] += dot(pb[...], do_all[i].reshape(group * chunk, dim))
                    elif h == 1:
                        dkv[at, 0] += dot(sb[...], q_all[i].reshape(group * chunk, dim))
                    for e in range(group):
                        if min(2 + e // (group // 2), group - 1) == h:
                            acc_t[:, cs(e)] += dot(kt[j2], sb[:, cs(e)])
                if k1 is not None:
                    p = jnp.exp2(s_scr[k1, :, cs(h)] - lse_scr[0:1, cs(h)])
                    buf1[0][:, cs(h)] = p.astype(BF16)
                    buf1[1][:, cs(h)] = (p * (dp_t - d_scr[0:1, cs(h)])).astype(BF16)

        grad(0, buf_a, None, None)

        def bwd_body(t, _):
            grad(2 * t + 1, buf_b, 2 * t, buf_a)
            grad(2 * t + 2, buf_a, 2 * t + 1, buf_b)

            @pl.when((i > 0) & (t == r // 2))
            def _():
                sib_copy(i).start()

            return 0

        lax.fori_loop(0, (n - 1) // 2, bwd_body, 0)

        @pl.when(odd)
        def _():
            grad(None, None, n - 1, buf_a)

        @pl.when(jnp.logical_not(odd))
        def _():
            grad(n - 1, buf_b, n - 2, buf_a)
            grad(None, None, n - 1, buf_b)

        for h in range(group):
            dq_st[i, h] = (acc_t[:, cs(h)] * sm_scale).astype(BF16).T

        @pl.when(i != y)
        def _():
            out_copies(i)[1].start()

        @pl.when(i == 0)
        def _():
            sib_copy(i).start()

        reduce_start(i)

        @pl.when(step == 0)
        def _():
            for s in slots[3:]:
                ready(s)
            for s in slots[1:]:
                for which in qdo:
                    wait_in(which, s)

        @pl.when(step > 0)
        def _():
            reduce_end(i + 1)

        return 0

    lax.fori_loop(0, n_y, one_chunk, 0)
    o_out[y] = o_st[y]
    dq_out[y] = dq_st[y]
    for d in yorder:
        for cp in [kv_copy(d)] + [qdo_copy(which, d) for which in qdo]:
            cp.wait_send()
    for s in slots:
        sb_copy(s, 0).wait_send()
        for dx in xorder:
            ag_copy(s, dx).wait_send()
            sb_copy(s, dx).wait_send()
    reduce_end(0)
    dkv_out[y] = dkv_st[y]
    for yy in range(n_y):
        @pl.when(yy != y)
        def _():
            for k, out in enumerate((o_out, dq_out)):
                rcopy(o_st.at[yy], out.at[yy], od_s.at[k, yy], od_r.at[k, yy], sib).wait_recv()
            rcopy(dkv_st.at[yy], dkv_out.at[yy], fy_s.at[yy], fy_r.at[yy], sib).wait_recv()
            for cp in out_copies(yy):
                cp.wait_send()
            y_copy(yy).wait_send()

        sib_copy(yy).wait_send()
        for dx in xorder:
            x_copy(yy, dx).wait_send()


def solution(mesh):
    n_ctx = mesh.shape['ctx']
    seq_spec = P('dp', 'ctx', None, None)

    def local_attn(q_loc, k_loc, v_loc, do_loc):
        n_batch, chunk, q_heads, dim = q_loc.shape
        kv_heads = k_loc.shape[2]
        group = q_heads // kv_heads
        inner = n_ctx // kv_heads
        n_x = inner // 2
        n_win = WINDOW // chunk
        n_y = kv_heads
        wide = group * chunk

        def heads(x, per):
            return jnp.transpose(x[0], (1, 0, 2)).reshape(kv_heads, per, chunk, dim)

        def tokens(x):
            return jnp.transpose(x.reshape(-1, chunk, dim), (1, 0, 2))[None]

        q4, do4 = heads(q_loc, group), heads(do_loc, group)
        kv4 = jnp.concatenate([heads(k_loc, 1), heads(v_loc, 1)], axis=1)
        vm = pl.BlockSpec(memory_space=pltpu.VMEM)
        dma = pltpu.SemaphoreType.DMA
        o4, dq4, dkv4 = pl.pallas_call(
            functools.partial(attn_kernel, inner, n_win, dim ** -0.5),
            out_shape=(jax.ShapeDtypeStruct(q4.shape, BF16), jax.ShapeDtypeStruct(q4.shape, BF16),
                       jax.ShapeDtypeStruct(kv4.shape, BF16)),
            in_specs=[vm] * 3,
            out_specs=(vm,) * 3,
            scratch_shapes=[
                pltpu.VMEM(q4.shape, BF16), pltpu.VMEM(q4.shape, BF16), pltpu.VMEM((n_ctx, 2, chunk, dim), BF16),
                pltpu.VMEM((n_ctx, dim, chunk), BF16), pltpu.VMEM((n_ctx, dim, chunk), BF16),
                pltpu.VMEM((dim, wide), BF16), pltpu.VMEM((dim, wide), BF16),
                pltpu.VMEM((n_win + 1, chunk, wide), F32), pltpu.VMEM((dim, wide), F32),
                pltpu.VMEM((8, wide), F32), pltpu.VMEM((8, wide), F32),
                pltpu.VMEM((8, wide), F32), pltpu.VMEM((8, wide), F32),
                pltpu.VMEM((chunk, wide), BF16), pltpu.VMEM((chunk, wide), BF16),
                pltpu.VMEM((chunk, wide), BF16), pltpu.VMEM((chunk, wide), BF16),
                pltpu.VMEM((n_ctx, 2, chunk, dim), F32), pltpu.VMEM(q4.shape, BF16), pltpu.VMEM(q4.shape, BF16),
                pltpu.VMEM((n_ctx // 2, 2, chunk, dim), F32), pltpu.VMEM((n_x, n_y, 2, chunk, dim), F32),
                pltpu.VMEM(kv4.shape, BF16),
                dma((3,)), dma((3, n_y)), dma((3, n_y)), dma((n_y, n_x)), dma((n_y, n_x)), dma((n_y, n_x)), dma((n_y, n_x)),
                dma((2, n_y)), dma((2, n_y)), dma((n_y,)), dma((n_y,)), dma((n_y, n_x)), dma((n_y, n_x)),
                dma((n_y,)), dma((n_y,)),
            ],
            compiler_params=pltpu.CompilerParams(vmem_limit_bytes=63 * 1024 * 1024, collective_id=0, has_side_effects=True),
            name='attn_core',
        )(q4, do4, kv4)
        return tokens(o4), tokens(dq4), tokens(dkv4[:, 0]), tokens(dkv4[:, 1])

    return jax.shard_map(local_attn, mesh=mesh, in_specs=(seq_spec,) * 4, out_specs=(seq_spec,) * 4, check_vma=False)
```

```python
import functools

import jax
import jax.numpy as jnp
from jax import lax
from jax.experimental import pallas as pl
from jax.experimental.pallas import tpu as pltpu
from jax.sharding import PartitionSpec as P

WINDOW = 4096
NEG = -1e30
LOG2E = 1.4426950408889634
F32 = jnp.float32
BF16 = jnp.bfloat16


def dot(a, b):
    return jnp.dot(a, b, preferred_element_type=F32)


def fold8(x, op):
    n = x.shape[0] // 8
    acc = x[0:8]
    for t in range(1, n):
        acc = op(acc, x[8 * t:8 * t + 8])
    return acc


MESH = pl.DeviceIdType.MESH


def attn_kernel(inner, n_win, sm_scale, q_loc, do_loc, kv_loc, o_out, dq_out, dkv_out,
                q_all, do_all, kv_all, kt, vt, qt, dot_t, s_scr, acc_t, m_scr, l_scr, lse_scr, d_scr,
                p_a, s_a, p_b, s_b, dkv, o_st, dq_st, sib_in, x_in, dkv_st,
                loc_sem, in_s, in_r, ag_s, ag_r, sb_s, sb_r, od_s, od_r, ds_s, ds_r, xs_s, xs_r, fy_s, fy_r):
    n_y, group, chunk, dim = q_loc.shape
    n_kv = kv_all.shape[0]
    n_x = inner // 2
    half = n_kv // 2
    top = n_y - 1
    dp = lax.axis_index('dp')
    me = lax.axis_index('ctx')
    y, r = me // inner, lax.rem(me, inner)
    x, c = r // 2, lax.rem(r, 2)
    c_exp = sm_scale * LOG2E

    def dev(yy, xx, cc):
        return (dp, yy * inner + xx * 2 + cc)

    def y_at(dy):
        return lax.rem(y + dy + n_y, n_y)

    def x_at(dx):
        return lax.rem(x + dx + n_x, n_x)

    def rcopy(src, dst, s, rr, to):
        return pltpu.make_async_remote_copy(src_ref=src, dst_ref=dst, send_sem=s, recv_sem=rr, device_id=to, device_id_type=MESH)

    sib = dev(y, x, 1 - c)
    peers = [dev(y_at(d), x, c) for d in range(1, n_y)] + [dev(y, x_at(d), c) for d in range(1, n_x)] + [sib]
    barrier = pltpu.get_barrier_semaphore()
    for p in peers:
        pl.semaphore_signal(barrier, inc=1, device_id=p, device_id_type=MESH)
    pl.semaphore_wait(barrier, len(peers))

    yorder = [1, n_y - 1] + list(range(2, n_y - 1))
    xorder = [1, n_x - 1] + list(range(2, n_x - 1))
    mine = y * inner + r
    locs = [pltpu.make_async_copy(kv_loc.at[y], kv_all.at[mine], loc_sem.at[0]),
            pltpu.make_async_copy(q_loc.at[y], q_all.at[y], loc_sem.at[1]),
            pltpu.make_async_copy(do_loc.at[y], do_all.at[y], loc_sem.at[2])]
    for cp in locs:
        cp.start()

    def kv_copy(d):
        return rcopy(kv_loc.at[y_at(d)], kv_all.at[mine], in_s.at[0, d], in_r.at[0, d], dev(y_at(d), x, c))

    qdo = ((1, q_loc, q_all), (2, do_loc, do_all))

    def qdo_copy(which, d):
        k, src, dst = which
        return rcopy(src.at[y_at(d)], dst.at[y], in_s.at[k, d], in_r.at[k, d], dev(y_at(d), x, c))

    def send_qdo():
        for which in qdo:
            qdo_copy(which, 1).start()
        for which in qdo:
            for d in yorder[1:]:
                qdo_copy(which, d).start()

    def wait_in(which, i):
        k, _, dst = which
        d = y_at(-i)
        rcopy(dst.at[i], dst.at[i], in_s.at[k, d], in_r.at[k, d], sib).wait_recv()

    lag = jnp.where(y == 0, 1, 0)
    top_first = jnp.where(y == 0, top, y)

    def back(k):
        return lax.rem(k + lag, n_y)

    def ag_copy(k, dx):
        idx = y_at(-back(k)) * inner + r
        return rcopy(kv_all.at[idx], kv_all.at[idx], ag_s.at[k, dx], ag_r.at[k, dx], dev(y, x_at(dx), c))

    def sb_copy(k, dx):
        idx = y_at(-back(k)) * inner + x_at(-dx) * 2 + c
        return rcopy(kv_all.at[idx], kv_all.at[idx], sb_s.at[k, dx], sb_r.at[k, dx], sib)

    for d in yorder:
        kv_copy(d).start()
    send_qdo()
    locs[0].wait()
    for k in range(n_y):
        @pl.when(back(k) > 0)
        def _():
            kk = back(k)
            idx = y_at(-kk) * inner + r
            rcopy(kv_all.at[idx], kv_all.at[idx], in_s.at[0, kk], in_r.at[0, kk], sib).wait_recv()

        for dx in xorder:
            ag_copy(k, dx).start()
        sb_copy(k, 0).start()

    def ready(k):
        s = y_at(-back(k))
        for dx in xorder:
            idx = s * inner + x_at(-dx) * 2 + c
            rcopy(kv_all.at[idx], kv_all.at[idx], ag_s.at[k, dx], ag_r.at[k, dx], sib).wait_recv()
            sb_copy(k, dx).start()
        for dx in [0] + xorder:
            idx = s * inner + x_at(-dx) * 2 + 1 - c
            rcopy(kv_all.at[idx], kv_all.at[idx], sb_s.at[k, dx], sb_r.at[k, dx], sib).wait_recv()

        def prep(t, _):
            j = s * inner + t
            kt[j] = kv_all[j, 0].T
            vt[j] = kv_all[j, 1].T
            dkv[lax.rem(j, 2) * half + j // 2] = jnp.zeros((2, chunk, dim), F32)
            return 0

        lax.fori_loop(0, inner, prep, 0)

    ready(0)

    @pl.when(r == 0)
    def _():
        ready(1)

    locs[1].wait()
    locs[2].wait()

    need_1 = (r + 1) // 2
    need_2 = (r + inner + 1) // 2
    diff = lax.broadcasted_iota(jnp.int32, (chunk, chunk), 0) - lax.broadcasted_iota(jnp.int32, (chunk, chunk), 1)

    def cs(h):
        return slice(h * chunk, (h + 1) * chunk)

    def out_copies(i):
        return [rcopy(st.at[i], out.at[y], od_s.at[k, i], od_r.at[k, y], dev(i, x, c))
                for k, (st, out) in enumerate(((o_st, o_out), (dq_st, dq_out)))]

    def sib_copy(i):
        return rcopy(dkv.at[pl.ds((1 - c) * half + n_x * i, n_x)], sib_in.at[pl.ds(n_x * i, n_x)], ds_s.at[i], ds_r.at[i], sib)

    xa = x + 1 - 2 * lax.rem(x, 2)
    xb = n_x - 1 - x

    def pairs(i):
        at = c * half + n_x * i
        first, second = (xa, n_x - 1 - xa, xb), (xb, xb + 1 - 2 * lax.rem(xb, 2), xa)
        out = []
        for which, (near, far, mid) in enumerate((first, second)):
            sems = lambda q: (xs_s.at[i, 3 * which + q], xs_r.at[i, 3 * which + q])
            out.append([rcopy(dkv.at[at + near, which], x_in.at[0, i, which], *sems(0), dev(y, near, c)),
                        rcopy(dkv.at[at + far, which], x_in.at[1, i, which], *sems(1), dev(y, near, c)),
                        rcopy(dkv.at[at + mid, which], x_in.at[2, i, which], *sems(2), dev(y, mid, c))])
        return out

    def y_copy(i):
        return rcopy(dkv_st.at[i], dkv_out.at[y], fy_s.at[i], fy_r.at[y], dev(i, x, c))

    def reduce_start(i):
        sib_copy(i).wait_recv()

        def add(t, _):
            at = c * half + n_x * i + t
            dkv[at] = dkv[at] + sib_in[n_x * i + t]
            return 0

        lax.fori_loop(0, n_x, add, 0)
        for q in (1, 0):
            for cps in pairs(i):
                cps[q].start()

    def reduce_mid(i):
        at = c * half + n_x * i
        for which, cps in enumerate(pairs(i)):
            mid = (xb, xa)[which]
            cps[1].wait_recv()
            dkv[at + mid, which] = dkv[at + mid, which] + x_in[1, i, which]
            cps[2].start()
        for which, cps in enumerate(pairs(i)):
            cps[0].wait_recv()
            dkv[at + x, which] = dkv[at + x, which] + x_in[0, i, which]

    def reduce_end(i):
        for cps in pairs(i):
            cps[2].wait_recv()
        tot = dkv[c * half + n_x * i + x] + x_in[2, i]
        dkv_st[i, 0] = (tot[0] * sm_scale).astype(BF16)
        dkv_st[i, 1] = tot[1].astype(BF16)

        @pl.when(i != y)
        def _():
            y_copy(i).start()

    def later_of(step):
        return jnp.where(n_y - step > top_first, n_y - step, top - step)

    def one_chunk(step, _):
        i = jnp.where(step == 0, top_first, later_of(step))
        g = i * inner + r

        @pl.when(i != y)
        def _():
            wait_in(qdo[0], i)

        n = jnp.maximum(jnp.minimum(g, n_win) + 1, 2)
        for h in range(group):
            qt[:, cs(h)] = q_all[i, h].T
        m_scr[...] = jnp.full(m_scr.shape, NEG, F32)
        l_scr[...] = jnp.zeros(l_scr.shape, F32)
        lse_scr[...] = jnp.full(lse_scr.shape, NEG, F32)
        acc_t[...] = jnp.zeros(acc_t.shape, F32)

        def key_of(k):
            return jnp.maximum(g - k, 0)

        def score(h, blocks):
            return [dot(kv_all[key_of(k), 0], qt[:, cs(h)]) for k, _ in blocks]

        def keep_score(h, blocks, scores):
            mx = m_scr[:, cs(h)]
            for (k, keep), s in zip(blocks, scores):
                s = s * c_exp
                if keep is not None:
                    s = jnp.where(keep, s, NEG)
                s_scr[k, :, cs(h)] = s
                mx = jnp.maximum(mx, fold8(s, jnp.maximum))
            m_scr[:, cs(h)] = mx

        def softmax_pv(h, blocks, m_new):
            m_old = lse_scr[:, cs(h)]
            alpha = jnp.exp2(m_old - m_new)
            lse_scr[:, cs(h)] = m_new
            l_new = l_scr[:, cs(h)] * alpha
            pv = None
            for k, _ in blocks:
                p = jnp.exp2(s_scr[k, :, cs(h)] - m_new[0:1])
                l_new = l_new + fold8(p, jnp.add)
                part = dot(vt[key_of(k)], p.astype(BF16))
                pv = part if pv is None else pv + part
            l_scr[:, cs(h)] = l_new
            acc_t[:, cs(h)] = acc_t[:, cs(h)] * alpha[0:1] + pv

        def row_max(h):
            m = m_scr[:, cs(h)]
            return jnp.broadcast_to(jnp.max(m, axis=0, keepdims=True), m.shape)

        def fwd(new, old):
            if old:
                m_new = [row_max(h) for h in range(group)]
            for h in range(group):
                if new:
                    scores = score(h, new)
                if old:
                    softmax_pv(h, old, m_new[h])
                if new:
                    keep_score(h, new, scores)

        def pair(p):
            return [(2 * p, None), (2 * p + 1, None)]

        n_pair = n // 2
        odd = lax.rem(n, 2) == 1
        last = [(n - 1, diff > jnp.where(g >= n_win, 0, -2 * chunk))]
        fwd([(0, diff <= 0), (1, diff < jnp.where(g > 0, 2 * chunk, -2 * chunk))], None)

        def fwd_body(p, _):
            @pl.when((step == 0) & (p == need_1))
            def _():
                ready(1)

            @pl.when((step == 0) & (top_first > 1) & (p == need_2))
            def _():
                ready(2)

            fwd(pair(p), pair(p - 1))
            return 0

        lax.fori_loop(1, n_pair, fwd_body, 0)

        @pl.when(odd)
        def _():
            @pl.when((step == 0) & (top_first > 1) & (n_pair == need_2))
            def _():
                ready(2)

            fwd(last, pair(n_pair - 1))
            fwd(None, last)

        @pl.when(jnp.logical_not(odd))
        def _():
            fwd(None, pair(n_pair - 1))

        @pl.when(i != y)
        def _():
            wait_in(qdo[1], i)

        for h in range(group):
            dot_t[:, cs(h)] = do_all[i, h].T
        l_row = jnp.sum(l_scr[...], axis=0, keepdims=True)
        lse_scr[...] = lse_scr[...] + jnp.log2(l_row)
        for h in range(group):
            o_t = (acc_t[:, cs(h)] / l_row[:, cs(h)]).astype(BF16)
            d = jnp.sum(o_t.astype(F32) * dot_t[:, cs(h)].astype(F32), axis=0, keepdims=True)
            d_scr[:, cs(h)] = jnp.broadcast_to(d, (8, chunk))
            o_st[i, h] = o_t.T
        acc_t[...] = jnp.zeros(acc_t.shape, F32)

        @pl.when(i != y)
        def _():
            out_copies(i)[0].start()

        own_last = (i != top_first) | (top_first == top)

        before = jnp.where(step == 1, top_first, later_of(step - 1))

        @pl.when((step > 0) & ((before != top_first) | (top_first == top)))
        def _():
            reduce_mid(before)

        @pl.when((step > 1) & (top_first < top) & (later_of(step - 1) == y + 1))
        def _():
            reduce_start(y)

        buf_a, buf_b = (p_a, s_a), (p_b, s_b)

        def grad(k1, buf1, k2, buf2):
            if k1 is not None:
                j1 = key_of(k1)
            if k2 is not None:
                j2 = key_of(k2)
                at = lax.rem(j2, 2) * half + j2 // 2
                pb, sb = buf2
            for h in range(group):
                if k1 is not None:
                    dp_t = dot(kv_all[j1, 1], dot_t[:, cs(h)])
                if k2 is not None:
                    if h == 0:
                        dkv[at, 1] += dot(pb[...], do_all[i].reshape(group * chunk, dim))
                    elif h == 1:
                        dkv[at, 0] += dot(sb[...], q_all[i].reshape(group * chunk, dim))
                    for e in range(group):
                        if min(2 + e // (group // 2), group - 1) == h:
                            acc_t[:, cs(e)] += dot(kt[j2], sb[:, cs(e)])
                if k1 is not None:
                    p = jnp.exp2(s_scr[k1, :, cs(h)] - lse_scr[0:1, cs(h)])
                    buf1[0][:, cs(h)] = p.astype(BF16)
                    buf1[1][:, cs(h)] = (p * (dp_t - d_scr[0:1, cs(h)])).astype(BF16)

        grad(0, buf_a, None, None)

        def bwd_body(t, _):
            grad(2 * t + 1, buf_b, 2 * t, buf_a)
            grad(2 * t + 2, buf_a, 2 * t + 1, buf_b)

            @pl.when(own_last & (i > 0) & (t == r // 2))
            def _():
                sib_copy(i).start()

            @pl.when(own_last & (i > 0) & (t == r // 2 + 2))
            def _():
                reduce_start(i)

            return 0

        lax.fori_loop(0, (n - 1) // 2, bwd_body, 0)

        @pl.when(odd)
        def _():
            grad(None, None, n - 1, buf_a)

        @pl.when(jnp.logical_not(odd))
        def _():
            grad(n - 1, buf_b, n - 2, buf_a)
            grad(None, None, n - 1, buf_b)

        for h in range(group):
            dq_st[i, h] = (acc_t[:, cs(h)] * sm_scale).astype(BF16).T

        @pl.when(i != y)
        def _():
            out_copies(i)[1].start()

        @pl.when(own_last & (i == 0))
        def _():
            sib_copy(i).start()

        @pl.when((step > 1) & (top_first < top) & (later_of(step - 1) == y + 1))
        def _():
            reduce_mid(y)

        @pl.when(own_last & (i == 0))
        def _():
            reduce_start(i)

        @pl.when((top_first < top) & (i == y + 1))
        def _():
            sib_copy(y).start()

        @pl.when(step == 0)
        def _():
            @pl.when(top_first < 2)
            def _():
                ready(2)

            ready(3)

        for late in range(2, n_y):
            @pl.when(step == late)
            def _():
                reduce_end(n_y + 1 - late)

        return 0

    lax.fori_loop(0, n_y, one_chunk, 0)

    reduce_mid(0)
    o_out[y] = o_st[y]
    dq_out[y] = dq_st[y]
    for d in yorder:
        for cp in [kv_copy(d)] + [qdo_copy(which, d) for which in qdo]:
            cp.wait_send()
    for k in range(n_y):
        sb_copy(k, 0).wait_send()
        for dx in xorder:
            ag_copy(k, dx).wait_send()
            sb_copy(k, dx).wait_send()
    reduce_end(1)
    reduce_end(0)
    dkv_out[y] = dkv_st[y]
    for yy in range(n_y):
        @pl.when(yy != y)
        def _():
            for k, out in enumerate((o_out, dq_out)):
                rcopy(o_st.at[yy], out.at[yy], od_s.at[k, yy], od_r.at[k, yy], sib).wait_recv()
            rcopy(dkv_st.at[yy], dkv_out.at[yy], fy_s.at[yy], fy_r.at[yy], sib).wait_recv()
            for cp in out_copies(yy):
                cp.wait_send()
            y_copy(yy).wait_send()

        sib_copy(yy).wait_send()
        for cps in pairs(yy):
            for cp in cps:
                cp.wait_send()


def solution(mesh):
    n_ctx = mesh.shape['ctx']
    seq_spec = P('dp', 'ctx', None, None)

    def local_attn(q_loc, k_loc, v_loc, do_loc):
        n_batch, chunk, q_heads, dim = q_loc.shape
        kv_heads = k_loc.shape[2]
        group = q_heads // kv_heads
        inner = n_ctx // kv_heads
        n_x = inner // 2
        n_win = WINDOW // chunk
        n_y = kv_heads
        wide = group * chunk

        def heads(x, per):
            return jnp.transpose(x[0], (1, 0, 2)).reshape(kv_heads, per, chunk, dim)

        def tokens(x):
            return jnp.transpose(x.reshape(-1, chunk, dim), (1, 0, 2))[None]

        q4, do4 = heads(q_loc, group), heads(do_loc, group)
        kv4 = jnp.concatenate([heads(k_loc, 1), heads(v_loc, 1)], axis=1)
        vm = pl.BlockSpec(memory_space=pltpu.VMEM)
        dma = pltpu.SemaphoreType.DMA
        o4, dq4, dkv4 = pl.pallas_call(
            functools.partial(attn_kernel, inner, n_win, dim ** -0.5),
            out_shape=(jax.ShapeDtypeStruct(q4.shape, BF16), jax.ShapeDtypeStruct(q4.shape, BF16),
                       jax.ShapeDtypeStruct(kv4.shape, BF16)),
            in_specs=[vm] * 3,
            out_specs=(vm,) * 3,
            scratch_shapes=[
                pltpu.VMEM(q4.shape, BF16), pltpu.VMEM(q4.shape, BF16), pltpu.VMEM((n_ctx, 2, chunk, dim), BF16),
                pltpu.VMEM((n_ctx, dim, chunk), BF16), pltpu.VMEM((n_ctx, dim, chunk), BF16),
                pltpu.VMEM((dim, wide), BF16), pltpu.VMEM((dim, wide), BF16),
                pltpu.VMEM((n_win + 1, chunk, wide), F32), pltpu.VMEM((dim, wide), F32),
                pltpu.VMEM((8, wide), F32), pltpu.VMEM((8, wide), F32),
                pltpu.VMEM((8, wide), F32), pltpu.VMEM((8, wide), F32),
                pltpu.VMEM((chunk, wide), BF16), pltpu.VMEM((chunk, wide), BF16),
                pltpu.VMEM((chunk, wide), BF16), pltpu.VMEM((chunk, wide), BF16),
                pltpu.VMEM((n_ctx, 2, chunk, dim), F32), pltpu.VMEM(q4.shape, BF16), pltpu.VMEM(q4.shape, BF16),
                pltpu.VMEM((n_ctx // 2, 2, chunk, dim), F32), pltpu.VMEM((n_x, n_y, 2, chunk, dim), F32),
                pltpu.VMEM(kv4.shape, BF16),
                dma((3,)), dma((3, n_y)), dma((3, n_y)), dma((n_y, n_x)), dma((n_y, n_x)), dma((n_y, n_x)), dma((n_y, n_x)),
                dma((2, n_y)), dma((2, n_y)), dma((n_y,)), dma((n_y,)), dma((n_y, 6)), dma((n_y, 6)),
                dma((n_y,)), dma((n_y,)),
            ],
            compiler_params=pltpu.CompilerParams(vmem_limit_bytes=63 * 1024 * 1024, collective_id=0, has_side_effects=True),
            name='attn_core',
        )(q4, do4, kv4)
        return tokens(o4), tokens(dq4), tokens(dkv4[:, 0]), tokens(dkv4[:, 1])

    return jax.shard_map(local_attn, mesh=mesh, in_specs=(seq_spec,) * 4, out_specs=(seq_spec,) * 4, check_vma=False)
```

```python
import functools

import jax
import jax.numpy as jnp
from jax import lax
from jax.experimental import pallas as pl
from jax.experimental.pallas import tpu as pltpu
from jax.sharding import PartitionSpec as P

WINDOW = 4096
NEG = -1e30
LOG2E = 1.4426950408889634
F32 = jnp.float32
BF16 = jnp.bfloat16


def dot(a, b):
    return jnp.dot(a, b, preferred_element_type=F32)


def fold8(x, op):
    n = x.shape[0] // 8
    acc = x[0:8]
    for t in range(1, n):
        acc = op(acc, x[8 * t:8 * t + 8])
    return acc


MESH = pl.DeviceIdType.MESH


def attn_kernel(inner, n_win, sm_scale, q_loc, do_loc, kv_loc, o_out, dq_out, dkv_out,
                q_all, do_all, kv_all, kt, vt, qt, dot_t, s_scr, acc_t, m_scr, l_scr, lse_scr, d_scr,
                p_a, s_a, p_b, s_b, dkv, o_st, dq_st, sib_in, x_in, dkv_st,
                loc_sem, in_s, in_r, ag_s, ag_r, sb_s, sb_r, od_s, od_r, ds_s, ds_r, xs_s, xs_r, fy_s, fy_r):
    n_y, group, chunk, dim = q_loc.shape
    n_kv = kv_all.shape[0]
    n_x = inner // 2
    half = n_kv // 2
    top = n_y - 1
    dp = lax.axis_index('dp')
    me = lax.axis_index('ctx')
    y, r = me // inner, lax.rem(me, inner)
    x, c = r // 2, lax.rem(r, 2)
    c_exp = sm_scale * LOG2E

    def dev(yy, xx, cc):
        return (dp, yy * inner + xx * 2 + cc)

    def y_at(dy):
        return lax.rem(y + dy + n_y, n_y)

    def x_at(dx):
        return lax.rem(x + dx + n_x, n_x)

    def rcopy(src, dst, s, rr, to):
        return pltpu.make_async_remote_copy(src_ref=src, dst_ref=dst, send_sem=s, recv_sem=rr, device_id=to, device_id_type=MESH)

    sib = dev(y, x, 1 - c)
    peers = [dev(y_at(d), x, c) for d in range(1, n_y)] + [dev(y, x_at(d), c) for d in range(1, n_x)] + [sib]
    barrier = pltpu.get_barrier_semaphore()
    for p in peers:
        pl.semaphore_signal(barrier, inc=1, device_id=p, device_id_type=MESH)
    pl.semaphore_wait(barrier, len(peers))

    yorder = [1, n_y - 1] + list(range(2, n_y - 1))
    xorder = [1, n_x - 1] + list(range(2, n_x - 1))
    mine = y * inner + r
    locs = [pltpu.make_async_copy(kv_loc.at[y], kv_all.at[mine], loc_sem.at[0]),
            pltpu.make_async_copy(q_loc.at[y], q_all.at[y], loc_sem.at[1]),
            pltpu.make_async_copy(do_loc.at[y], do_all.at[y], loc_sem.at[2])]
    for cp in locs:
        cp.start()

    def kv_copy(d):
        return rcopy(kv_loc.at[y_at(d)], kv_all.at[mine], in_s.at[0, d], in_r.at[0, d], dev(y_at(d), x, c))

    qdo = ((1, q_loc, q_all), (2, do_loc, do_all))

    def qdo_copy(which, d):
        k, src, dst = which
        return rcopy(src.at[y_at(d)], dst.at[y], in_s.at[k, d], in_r.at[k, d], dev(y_at(d), x, c))

    def send_qdo():
        for which in qdo:
            qdo_copy(which, 1).start()
        for which in qdo:
            for d in yorder[1:]:
                qdo_copy(which, d).start()

    def wait_in(which, i):
        k, _, dst = which
        d = y_at(-i)
        rcopy(dst.at[i], dst.at[i], in_s.at[k, d], in_r.at[k, d], sib).wait_recv()

    lag = jnp.where(y == 0, 1, 0)
    top_first = jnp.where(y == 0, top, y)

    def back(k):
        return lax.rem(k + lag, n_y)

    def ag_copy(k, dx):
        idx = y_at(-back(k)) * inner + r
        return rcopy(kv_all.at[idx], kv_all.at[idx], ag_s.at[k, dx], ag_r.at[k, dx], dev(y, x_at(dx), c))

    def sb_copy(k, dx):
        idx = y_at(-back(k)) * inner + x_at(-dx) * 2 + c
        return rcopy(kv_all.at[idx], kv_all.at[idx], sb_s.at[k, dx], sb_r.at[k, dx], sib)

    for d in yorder:
        kv_copy(d).start()
    send_qdo()
    locs[0].wait()
    for k in range(n_y):
        @pl.when(back(k) > 0)
        def _():
            kk = back(k)
            idx = y_at(-kk) * inner + r
            rcopy(kv_all.at[idx], kv_all.at[idx], in_s.at[0, kk], in_r.at[0, kk], sib).wait_recv()

        for dx in xorder:
            ag_copy(k, dx).start()
        sb_copy(k, 0).start()

    def ready(k):
        s = y_at(-back(k))
        for dx in xorder:
            idx = s * inner + x_at(-dx) * 2 + c
            rcopy(kv_all.at[idx], kv_all.at[idx], ag_s.at[k, dx], ag_r.at[k, dx], sib).wait_recv()
            sb_copy(k, dx).start()
        for dx in [0] + xorder:
            idx = s * inner + x_at(-dx) * 2 + 1 - c
            rcopy(kv_all.at[idx], kv_all.at[idx], sb_s.at[k, dx], sb_r.at[k, dx], sib).wait_recv()

        def prep(t, _):
            j = s * inner + t
            kt[j] = kv_all[j, 0].T
            vt[j] = kv_all[j, 1].T
            dkv[lax.rem(j, 2) * half + j // 2] = jnp.zeros((2, chunk, dim), F32)
            return 0

        lax.fori_loop(0, inner, prep, 0)

    ready(0)

    @pl.when(r == 0)
    def _():
        ready(1)

    locs[1].wait()
    locs[2].wait()

    need_1 = (r + 1) // 2
    need_2 = (r + inner + 1) // 2
    diff = lax.broadcasted_iota(jnp.int32, (chunk, chunk), 0) - lax.broadcasted_iota(jnp.int32, (chunk, chunk), 1)

    def cs(h):
        return slice(h * chunk, (h + 1) * chunk)

    def out_copies(i):
        return [rcopy(st.at[i], out.at[y], od_s.at[k, i], od_r.at[k, y], dev(i, x, c))
                for k, (st, out) in enumerate(((o_st, o_out), (dq_st, dq_out)))]

    def sib_copy(i):
        return rcopy(dkv.at[pl.ds((1 - c) * half + n_x * i, n_x)], sib_in.at[pl.ds(n_x * i, n_x)], ds_s.at[i], ds_r.at[i], sib)

    xa = x + 1 - 2 * lax.rem(x, 2)
    xb = n_x - 1 - x

    def pairs(i):
        at = c * half + n_x * i
        first, second = (xa, n_x - 1 - xa, xb), (xb, xb + 1 - 2 * lax.rem(xb, 2), xa)
        out = []
        for which, (near, far, mid) in enumerate((first, second)):
            sems = lambda q: (xs_s.at[i, 3 * which + q], xs_r.at[i, 3 * which + q])
            out.append([rcopy(dkv.at[at + near, which], x_in.at[0, i, which], *sems(0), dev(y, near, c)),
                        rcopy(dkv.at[at + far, which], x_in.at[1, i, which], *sems(1), dev(y, near, c)),
                        rcopy(dkv.at[at + mid, which], x_in.at[2, i, which], *sems(2), dev(y, mid, c))])
        return out

    def y_copy(i):
        return rcopy(dkv_st.at[i], dkv_out.at[y], fy_s.at[i], fy_r.at[y], dev(i, x, c))

    def reduce_start(i):
        sib_copy(i).wait_recv()
        (dk_near, dk_far, _), (dv_near, dv_far, _) = pairs(i)
        for t, cps in ((n_x - 1 - xa, (dk_far, dv_far)), (xa, (dk_near,)), (xb, (dv_near,)), (x, ())):
            at = c * half + n_x * i + t
            dkv[at] = dkv[at] + sib_in[n_x * i + t]
            for cp in cps:
                cp.start()

    def reduce_mid(i):
        at = c * half + n_x * i
        for which, cps in enumerate(pairs(i)):
            mid = (xb, xa)[which]
            cps[1].wait_recv()
            dkv[at + mid, which] = dkv[at + mid, which] + x_in[1, i, which]
            cps[2].start()
        for which, cps in enumerate(pairs(i)):
            cps[0].wait_recv()
            dkv[at + x, which] = dkv[at + x, which] + x_in[0, i, which]

    def reduce_end(i):
        for cps in pairs(i):
            cps[2].wait_recv()
        tot = dkv[c * half + n_x * i + x] + x_in[2, i]
        dkv_st[i, 0] = (tot[0] * sm_scale).astype(BF16)
        dkv_st[i, 1] = tot[1].astype(BF16)

        @pl.when(i != y)
        def _():
            y_copy(i).start()

    def later_of(step):
        return jnp.where(n_y - step > top_first, n_y - step, top - step)

    def one_chunk(step, _):
        i = jnp.where(step == 0, top_first, later_of(step))
        g = i * inner + r

        @pl.when(i != y)
        def _():
            wait_in(qdo[0], i)

        n = jnp.maximum(jnp.minimum(g, n_win) + 1, 2)
        for h in range(group):
            qt[:, cs(h)] = q_all[i, h].T
        m_scr[...] = jnp.full(m_scr.shape, NEG, F32)
        l_scr[...] = jnp.zeros(l_scr.shape, F32)
        lse_scr[...] = jnp.full(lse_scr.shape, NEG, F32)
        acc_t[...] = jnp.zeros(acc_t.shape, F32)

        def key_of(k):
            return jnp.maximum(g - k, 0)

        def score(h, blocks):
            return [dot(kv_all[key_of(k), 0], qt[:, cs(h)]) for k, _ in blocks]

        def keep_score(h, blocks, scores):
            mx = m_scr[:, cs(h)]
            for (k, keep), s in zip(blocks, scores):
                s = s * c_exp
                if keep is not None:
                    s = jnp.where(keep, s, NEG)
                s_scr[k, :, cs(h)] = s
                mx = jnp.maximum(mx, fold8(s, jnp.maximum))
            m_scr[:, cs(h)] = mx

        def softmax_pv(h, blocks, m_new):
            m_old = lse_scr[:, cs(h)]
            alpha = jnp.exp2(m_old - m_new)
            lse_scr[:, cs(h)] = m_new
            l_new = l_scr[:, cs(h)] * alpha
            pv = None
            for k, _ in blocks:
                p = jnp.exp2(s_scr[k, :, cs(h)] - m_new[0:1])
                l_new = l_new + fold8(p, jnp.add)
                part = dot(vt[key_of(k)], p.astype(BF16))
                pv = part if pv is None else pv + part
            l_scr[:, cs(h)] = l_new
            acc_t[:, cs(h)] = acc_t[:, cs(h)] * alpha[0:1] + pv

        def row_max(h):
            m = m_scr[:, cs(h)]
            return jnp.broadcast_to(jnp.max(m, axis=0, keepdims=True), m.shape)

        def fwd(new, old):
            if old:
                m_new = [row_max(h) for h in range(group)]
            for h in range(group):
                if new:
                    scores = score(h, new)
                if old:
                    softmax_pv(h, old, m_new[h])
                if new:
                    keep_score(h, new, scores)

        def pair(p):
            return [(2 * p, None), (2 * p + 1, None)]

        n_pair = n // 2
        odd = lax.rem(n, 2) == 1
        last = [(n - 1, diff > jnp.where(g >= n_win, 0, -2 * chunk))]
        fwd([(0, diff <= 0), (1, diff < jnp.where(g > 0, 2 * chunk, -2 * chunk))], None)

        def fwd_body(p, _):
            @pl.when((step == 0) & (p == need_1))
            def _():
                ready(1)

            @pl.when((step == 0) & (top_first > 1) & (p == need_2))
            def _():
                ready(2)

            fwd(pair(p), pair(p - 1))
            return 0

        lax.fori_loop(1, n_pair, fwd_body, 0)

        @pl.when(odd)
        def _():
            @pl.when((step == 0) & (top_first > 1) & (n_pair == need_2))
            def _():
                ready(2)

            fwd(last, pair(n_pair - 1))
            fwd(None, last)

        @pl.when(jnp.logical_not(odd))
        def _():
            fwd(None, pair(n_pair - 1))

        @pl.when(i != y)
        def _():
            wait_in(qdo[1], i)

        for h in range(group):
            dot_t[:, cs(h)] = do_all[i, h].T
        l_row = jnp.sum(l_scr[...], axis=0, keepdims=True)
        lse_scr[...] = lse_scr[...] + jnp.log2(l_row)
        for h in range(group):
            o_t = (acc_t[:, cs(h)] / l_row[:, cs(h)]).astype(BF16)
            d = jnp.sum(o_t.astype(F32) * dot_t[:, cs(h)].astype(F32), axis=0, keepdims=True)
            d_scr[:, cs(h)] = jnp.broadcast_to(d, (8, chunk))
            o_st[i, h] = o_t.T
        acc_t[...] = jnp.zeros(acc_t.shape, F32)

        @pl.when(i != y)
        def _():
            out_copies(i)[0].start()

        own_last = (i != top_first) | (top_first == top)

        before = jnp.where(step == 1, top_first, later_of(step - 1))

        @pl.when((step > 0) & ((before != top_first) | (top_first == top)))
        def _():
            reduce_mid(before)

        @pl.when((step > 1) & (top_first < top) & (later_of(step - 1) == y + 1))
        def _():
            reduce_start(y)

        buf_a, buf_b = (p_a, s_a), (p_b, s_b)

        def grad(k1, buf1, k2, buf2):
            if k1 is not None:
                j1 = key_of(k1)
            if k2 is not None:
                j2 = key_of(k2)
                at = lax.rem(j2, 2) * half + j2 // 2
                pb, sb = buf2
            for h in range(group):
                if k1 is not None:
                    dp_t = dot(kv_all[j1, 1], dot_t[:, cs(h)])
                if k2 is not None:
                    if h == 0:
                        dkv[at, 1] += dot(pb[...], do_all[i].reshape(group * chunk, dim))
                    elif h == 1:
                        dkv[at, 0] += dot(sb[...], q_all[i].reshape(group * chunk, dim))
                    for e in range(group):
                        if min(2 + e // (group // 2), group - 1) == h:
                            acc_t[:, cs(e)] += dot(kt[j2], sb[:, cs(e)])
                if k1 is not None:
                    p = jnp.exp2(s_scr[k1, :, cs(h)] - lse_scr[0:1, cs(h)])
                    buf1[0][:, cs(h)] = p.astype(BF16)
                    buf1[1][:, cs(h)] = (p * (dp_t - d_scr[0:1, cs(h)])).astype(BF16)

        grad(0, buf_a, None, None)

        def bwd_body(t, _):
            grad(2 * t + 1, buf_b, 2 * t, buf_a)
            grad(2 * t + 2, buf_a, 2 * t + 1, buf_b)

            @pl.when(own_last & (i > 0) & (t == r // 2))
            def _():
                sib_copy(i).start()

            @pl.when(own_last & (i > 0) & (t == r // 2 + 3))
            def _():
                reduce_start(i)

            return 0

        lax.fori_loop(0, (n - 1) // 2, bwd_body, 0)

        @pl.when(odd)
        def _():
            grad(None, None, n - 1, buf_a)

        @pl.when(jnp.logical_not(odd))
        def _():
            grad(n - 1, buf_b, n - 2, buf_a)
            grad(None, None, n - 1, buf_b)

        for h in range(group):
            dq_st[i, h] = (acc_t[:, cs(h)] * sm_scale).astype(BF16).T

        @pl.when(i != y)
        def _():
            out_copies(i)[1].start()

        @pl.when(own_last & (i == 0))
        def _():
            sib_copy(i).start()

        @pl.when((step > 1) & (top_first < top) & (later_of(step - 1) == y + 1))
        def _():
            reduce_mid(y)

        @pl.when(own_last & (i == 0))
        def _():
            reduce_start(i)

        @pl.when((top_first < top) & (i == y + 1))
        def _():
            sib_copy(y).start()

        @pl.when(step == 0)
        def _():
            @pl.when(top_first < 2)
            def _():
                ready(2)

            ready(3)

        for late in range(2, n_y):
            @pl.when(step == late)
            def _():
                reduce_end(n_y + 1 - late)

        return 0

    lax.fori_loop(0, n_y, one_chunk, 0)

    reduce_mid(0)
    o_out[y] = o_st[y]
    dq_out[y] = dq_st[y]
    for d in yorder:
        for cp in [kv_copy(d)] + [qdo_copy(which, d) for which in qdo]:
            cp.wait_send()
    for k in range(n_y):
        sb_copy(k, 0).wait_send()
        for dx in xorder:
            ag_copy(k, dx).wait_send()
            sb_copy(k, dx).wait_send()
    reduce_end(1)
    reduce_end(0)
    dkv_out[y] = dkv_st[y]
    for yy in range(n_y):
        @pl.when(yy != y)
        def _():
            for k, out in enumerate((o_out, dq_out)):
                rcopy(o_st.at[yy], out.at[yy], od_s.at[k, yy], od_r.at[k, yy], sib).wait_recv()
            rcopy(dkv_st.at[yy], dkv_out.at[yy], fy_s.at[yy], fy_r.at[yy], sib).wait_recv()
            for cp in out_copies(yy):
                cp.wait_send()
            y_copy(yy).wait_send()

        sib_copy(yy).wait_send()
        for cps in pairs(yy):
            for cp in cps:
                cp.wait_send()


def solution(mesh):
    n_ctx = mesh.shape['ctx']
    seq_spec = P('dp', 'ctx', None, None)

    def local_attn(q_loc, k_loc, v_loc, do_loc):
        n_batch, chunk, q_heads, dim = q_loc.shape
        kv_heads = k_loc.shape[2]
        group = q_heads // kv_heads
        inner = n_ctx // kv_heads
        n_x = inner // 2
        n_win = WINDOW // chunk
        n_y = kv_heads
        wide = group * chunk

        def heads(x, per):
            return jnp.transpose(x[0], (1, 0, 2)).reshape(kv_heads, per, chunk, dim)

        def tokens(x):
            return jnp.transpose(x.reshape(-1, chunk, dim), (1, 0, 2))[None]

        q4, do4 = heads(q_loc, group), heads(do_loc, group)
        kv4 = jnp.concatenate([heads(k_loc, 1), heads(v_loc, 1)], axis=1)
        vm = pl.BlockSpec(memory_space=pltpu.VMEM)
        dma = pltpu.SemaphoreType.DMA
        o4, dq4, dkv4 = pl.pallas_call(
            functools.partial(attn_kernel, inner, n_win, dim ** -0.5),
            out_shape=(jax.ShapeDtypeStruct(q4.shape, BF16), jax.ShapeDtypeStruct(q4.shape, BF16),
                       jax.ShapeDtypeStruct(kv4.shape, BF16)),
            in_specs=[vm] * 3,
            out_specs=(vm,) * 3,
            scratch_shapes=[
                pltpu.VMEM(q4.shape, BF16), pltpu.VMEM(q4.shape, BF16), pltpu.VMEM((n_ctx, 2, chunk, dim), BF16),
                pltpu.VMEM((n_ctx, dim, chunk), BF16), pltpu.VMEM((n_ctx, dim, chunk), BF16),
                pltpu.VMEM((dim, wide), BF16), pltpu.VMEM((dim, wide), BF16),
                pltpu.VMEM((n_win + 1, chunk, wide), F32), pltpu.VMEM((dim, wide), F32),
                pltpu.VMEM((8, wide), F32), pltpu.VMEM((8, wide), F32),
                pltpu.VMEM((8, wide), F32), pltpu.VMEM((8, wide), F32),
                pltpu.VMEM((chunk, wide), BF16), pltpu.VMEM((chunk, wide), BF16),
                pltpu.VMEM((chunk, wide), BF16), pltpu.VMEM((chunk, wide), BF16),
                pltpu.VMEM((n_ctx, 2, chunk, dim), F32), pltpu.VMEM(q4.shape, BF16), pltpu.VMEM(q4.shape, BF16),
                pltpu.VMEM((n_ctx // 2, 2, chunk, dim), F32), pltpu.VMEM((n_x, n_y, 2, chunk, dim), F32),
                pltpu.VMEM(kv4.shape, BF16),
                dma((3,)), dma((3, n_y)), dma((3, n_y)), dma((n_y, n_x)), dma((n_y, n_x)), dma((n_y, n_x)), dma((n_y, n_x)),
                dma((2, n_y)), dma((2, n_y)), dma((n_y,)), dma((n_y,)), dma((n_y, 6)), dma((n_y, 6)),
                dma((n_y,)), dma((n_y,)),
            ],
            compiler_params=pltpu.CompilerParams(vmem_limit_bytes=63 * 1024 * 1024, collective_id=0, has_side_effects=True),
            name='attn_core',
        )(q4, do4, kv4)
        return tokens(o4), tokens(dq4), tokens(dkv4[:, 0]), tokens(dkv4[:, 1])

    return jax.shard_map(local_attn, mesh=mesh, in_specs=(seq_spec,) * 4, out_specs=(seq_spec,) * 4, check_vma=False)
```
